32 devices in a mesh: fsdp: 16 (over z, y, x), tp: 2 (over core).
Axes of the slice: x: 2, y: 2, z: 4, core: 2. Of those that a mesh axis runs over, the one named last changes fastest.
Arguments:
- inputs: bfloat16 [4096, 4096], P('fsdp'), may hold values from -6 to 6
- value_grad: bfloat16 [4096, 1024], P('fsdp', 'tp'), may hold values from -24 to 24
- value_weight: bfloat16 [4096, 1024], P('tp', 'fsdp'), may hold values from -0.09375 to 0.09375
- counts: int32 [16, 4], P('fsdp'), may hold values from 1 to 232, as said below
- offsets: int32 [16, 4], P('fsdp'), may hold values from 0 to 248, as said below
Outputs:
- input_grad: bfloat16 [4096, 4096], P('fsdp', 'tp')
- weight_grad: float32 [4096, 1024], P('fsdp', 'tp')
The draws below stay inside these ranges and needn't reach their ends.
Inputs may be any that keep to these rules, and one draw needn't show every extreme that they name: `offsets`: on each index of fsdp the 4 samples lie in order; each starts at a multiple of 8, at or after the 8-row-aligned end of the previous one, and all lie within the 256 rows; on some index the aligned blocks of its samples fill all 256 rows. `counts`: how many rows the samples of a row group fill varies widely between indices of fsdp.
All inputs are finite; a program needn't handle non-finite values.
Results may differ from the reference program's by a relative error of at most 0.0046.
Values may be sent and summed in bfloat16 or wider, within the bound.
A program may use at most 64 MiB of HBM per device.

```python
import math
import jax
import jax.numpy as jnp
from jax import lax

D = 4096
KV = 1024
TOK_DEV = 256
S_DEV = 4
TOKENS = 4096
SAMPLES = 64
N_FSDP = 16


def packing_layout(key):
    units_all = TOK_DEV // 8
    spare = units_all - S_DEV
    divisor = max(spare, 1)
    first = jax.random.randint(jax.random.fold_in(key, 101), (N_FSDP,), 0, spare + 1)
    second = jax.random.randint(jax.random.fold_in(key, 102), (N_FSDP,), 0, spare + 1)
    extra = first * second // divisor
    chosen = jax.random.randint(jax.random.fold_in(key, 103), (), 0, N_FSDP)
    is_chosen = jnp.arange(N_FSDP) == chosen
    extra = jnp.where(is_chosen, spare, extra)
    raw_cuts = jax.random.randint(jax.random.fold_in(key, 104), (N_FSDP, S_DEV - 1), 0, spare + 1)
    cuts = jnp.sort(raw_cuts * extra[:, None] // divisor, axis=1)
    cuts = jnp.where(is_chosen[:, None], spare, cuts)
    edges = jnp.concatenate([jnp.zeros((N_FSDP, 1), jnp.int32), cuts.astype(jnp.int32), extra[:, None].astype(jnp.int32)], axis=1)
    units = 1 + edges[:, 1:] - edges[:, :-1]
    ends = jnp.cumsum(units, axis=1)
    offsets = (8 * (ends - units)).astype(jnp.int32)
    trims = jax.random.randint(jax.random.fold_in(key, 105), (N_FSDP, S_DEV), 0, 8)
    slots = jnp.arange(S_DEV)[None, :]
    fixed_trims = jnp.where(slots == S_DEV - 1, 7, 0)
    trims = jnp.where(is_chosen[:, None], fixed_trims, trims)
    counts = (8 * units - trims).astype(jnp.int32)
    return (counts, offsets)


def draw_counts(key, part):
    return packing_layout(key)[0]


def draw_offsets(key, part):
    return packing_layout(key)[1]


def strengthened(result, own_key, source, target, shards_of, factor):
    def block_of(dim):
        return (jnp.arange(result.shape[dim]) // (result.shape[dim] // shards_of)).reshape((-1,) + (1,) * (result.ndim - 1 - dim))

    near = jax.random.permutation(own_key, shards_of)[block_of(target)]
    second = (block_of(target) + shards_of // 2) % shards_of
    return jnp.where((block_of(source) == near) | (block_of(source) == second), factor * result, result)


def block_scale(key, extent, cuts, low, high):
    factor_of = 1.0
    for position, parts in cuts:
        heights = jax.random.uniform(jax.random.fold_in(jax.random.fold_in(key, 6), position), (parts,), jnp.float32, low / len(cuts), high / len(cuts))
        factor_of = factor_of * jnp.repeat(jnp.exp(heights), extent[position] // parts).reshape((-1,) + (1,) * (len(extent) - 1 - position))
    return factor_of


def gaussian(stream_key, shape, width, most, pieces=(), kind=jnp.bfloat16):
    level = block_scale(stream_key, shape, pieces, -0.22, 0.18) if pieces else 1.0
    entries = jax.random.normal(stream_key, shape, jnp.float32) * width * level
    return jnp.minimum(jnp.maximum(entries, -most), most).astype(kind)


def heavy_noise(stream_key, shape, deviation, limit, cuts, heavy, kind=jnp.bfloat16):
    result = deviation * jax.random.normal(stream_key, shape, jnp.float32)
    if cuts:
        result = result * block_scale(stream_key, shape, cuts, -0.22, 0.18)
    return jnp.clip(strengthened(result, jax.random.fold_in(stream_key, 3), *heavy), -limit, limit).astype(kind)


def setup_inputs(seed: int = 0) -> dict:
    keys = jax.random.split(jax.random.key(seed), 6)
    inputs = heavy_noise(keys[0], (TOKENS, D), 1.0, 6.0, ((0, 16),), (0, 1, 16, 2.0))
    value_grad = gaussian(keys[1], (TOKENS, KV), 4.0, 24.0, ((0, 16), (1, 2)))
    value_weight = gaussian(keys[2], (D, KV), D ** -0.5, 0.09375, ((0, 2), (1, 16)))
    counts = draw_counts(jax.random.fold_in(keys[5], 71), 0)
    offsets = draw_offsets(jax.random.fold_in(keys[5], 71), 0)
    return {"inputs": inputs, "value_grad": value_grad, "value_weight": value_weight, "counts": counts, "offsets": offsets}


def reference(inputs, value_grad, value_weight, counts, offsets):
    positions = jnp.arange(TOK_DEV, dtype=jnp.int32)[None, :, None]
    inside = (positions >= offsets[:, None, :]) & (positions < offsets[:, None, :] + counts[:, None, :])
    inverse_root = lax.rsqrt(counts.astype(jnp.float32))[:, None, :]
    row_factor = lax.optimization_barrier(jnp.sum(jnp.where(inside, inverse_root, jnp.zeros_like(inverse_root)), axis=2))
    scaled = (value_grad.astype(jnp.float32).reshape(N_FSDP, TOK_DEV, KV) * row_factor[:, :, None]).astype(jnp.bfloat16)

    def rows_grad(group_rows):
        return jnp.dot(group_rows, value_weight.T, preferred_element_type=jnp.float32).astype(jnp.bfloat16)
    input_grad = lax.map(rows_grad, scaled).reshape(TOKENS, D)
    weight_grad = jnp.dot(inputs.T, scaled.reshape(TOKENS, KV), preferred_element_type=jnp.float32)
    weight_grad = weight_grad * (1.0 / math.sqrt(SAMPLES))
    return (input_grad, weight_grad)
```

```python
import functools
import math

import jax
import jax.numpy as jnp
from jax import lax
from jax.experimental import pallas as pl
from jax.experimental.pallas import tpu as pltpu
from jax.sharding import PartitionSpec as P

MESH = pl.DeviceIdType.MESH
GROUP = 4
VMEM_ROOM = 54 * 2**20


def scale_rows(value_grad, counts, offsets):
    positions = jnp.arange(value_grad.shape[0], dtype=jnp.int32)[:, None]
    starts = offsets[0][None, :]
    lengths = counts[0][None, :]
    inside = (positions >= starts) & (positions < starts + lengths)
    inverse_root = lax.rsqrt(lengths.astype(jnp.float32))
    row_factor = jnp.sum(jnp.where(inside, inverse_root, jnp.zeros_like(inverse_root)), axis=1)
    return (value_grad.astype(jnp.float32) * row_factor[:, None]).astype(jnp.bfloat16)


def general(inputs, value_grad, value_weight, counts, offsets):
    tok_rows = inputs.shape[0]
    row_block = min(128, tok_rows)
    scaled = scale_rows(value_grad, counts, offsets)
    live_end = jnp.max(offsets[0] + counts[0])
    live_blocks = (live_end + row_block - 1) // row_block
    scaled_all = lax.all_gather(scaled, "tp", axis=1, tiled=True)
    empty_inputs = jnp.zeros((tok_rows, value_weight.shape[0]), jnp.float32)
    piece = lax.all_gather(value_weight, "fsdp", axis=1, tiled=True)

    def add_add_block(block_index, partial_value):
        lower = lax.dynamic_slice_in_dim(scaled_all, block_index * row_block, row_block, 0)
        before = lax.dynamic_slice_in_dim(partial_value, block_index * row_block, row_block, 0)
        product = lax.dot_general(
            lower, piece, (((1,), (1,)), ((), ())), preferred_element_type=jnp.float32
        )
        return lax.dynamic_update_slice_in_dim(
            partial_value, before + product, block_index * row_block, 0
        )

    result = lax.fori_loop(0, live_blocks, add_add_block, empty_inputs)
    input_grad = result.astype(jnp.bfloat16)
    normalizer = 1.0 / math.sqrt(counts.shape[1] * lax.axis_size("fsdp"))
    empty = jnp.zeros((inputs.shape[1], scaled.shape[1]), jnp.float32)

    def weight_add_block(block_index, partial_value):
        feature_rows = lax.dynamic_slice_in_dim(inputs, block_index * row_block, row_block, 0)
        grad_rows = lax.dynamic_slice_in_dim(scaled, block_index * row_block, row_block, 0)
        return partial_value + lax.dot_general(
            feature_rows, grad_rows, (((0,), (0,)), ((), ())), preferred_element_type=jnp.float32
        )

    result = lax.fori_loop(0, live_blocks, weight_add_block, empty)
    summed = lax.psum_scatter(result, "fsdp", scatter_dimension=0, tiled=True)
    return (input_grad, summed * normalizer)


def kernel(
    n, normalizer, counts_ref, offsets_ref, x_hbm, g_hbm, wt_hbm, dx_ref, dw_ref,
    g_ref, wt_ref, x_src, s_all, x_all, w_all, acc, part_own, part_out, part_in, dx_out,
    local_sem, xf_sem, xo_sem, w_send, w_recv, s_send, s_recv, c_send, c_recv, x_send, x_recv,
    xs_send, xs_recv, g_send, g_recv, p_send, p_recv, o_send, o_recv,
):
    nz = n // GROUP
    me = lax.axis_index("fsdp")
    core = lax.axis_index("tp")
    sib = 1 - core
    z = me // GROUP
    quarter = me % GROUP
    dx = 1 - 2 * (me % 2)
    dy = 2 - 4 * ((me // 2) % 2)
    steps = (0, dx, dy, dx + dy)
    tok, half = g_ref.shape
    wcols = wt_ref.shape[0]
    fq = w_all.shape[1]
    hr = x_src.shape[3]
    upper = (2 * z) // nz
    order = [a + upper * (nz - 1 - 2 * a) for a in
             list(range(nz - 1, nz // 2 - 1, -1)) + list(range(nz // 2))]

    def remote(src, dst, send, recv, dev):
        return pltpu.make_async_remote_copy(
            src_ref=src, dst_ref=dst, send_sem=send, recv_sem=recv,
            device_id=dev, device_id_type=MESH,
        )

    def w_rows(f):
        return pl.ds(pl.multiple_of(f * wcols, wcols), wcols)

    def lanes(start, size):
        return pl.ds(pl.multiple_of(start, 128), size)

    def slot(j):
        return pl.ds(j * tok, tok)

    def x_lanes(i, q, h):
        return lanes(((order[i] * GROUP + q) * 2 + h) * hr, hr)

    fetch_w = pltpu.make_async_copy(wt_hbm, wt_ref, local_sem.at[0])
    fetch_own = pltpu.make_async_copy(
        wt_hbm.at[:, lanes(quarter * fq, fq)], w_all.at[w_rows(me), :], local_sem.at[1])
    fetch_g = pltpu.make_async_copy(g_hbm, g_ref, local_sem.at[2])
    for fetch in (fetch_w, fetch_own, fetch_g):
        fetch.start()

    barrier = pltpu.get_barrier_semaphore()
    for j in range(1, GROUP):
        pl.semaphore_signal(barrier, inc=1, device_id=(me + steps[j], core), device_id_type=MESH)
    pl.semaphore_signal(barrier, inc=1, device_id=(me, sib), device_id_type=MESH)
    ways = ((0, 1, z < nz - 1, z > 0), (1, -1, z > 0, z < nz - 1))
    for side, way, onward, behind in ways:
        @pl.when(onward)
        def _():
            pl.semaphore_signal(barrier, inc=1, device_id=(me + GROUP * way, core), device_id_type=MESH)

    x_fetches, own_fetches = {}, {}
    for i in range(nz):
        for j in (3, 1, 2):
            x_fetches[i, j] = pltpu.make_async_copy(
                x_hbm.at[:, x_lanes(i, quarter + steps[j], core)], x_src.at[i, j - 1], xf_sem.at[i, j - 1])
            x_fetches[i, j].start()
        for h in range(2):
            own_fetches[i, h] = pltpu.make_async_copy(
                x_hbm.at[:, x_lanes(i, quarter, h)], x_all.at[i, h, slot(0), :], xo_sem.at[i, h])
            own_fetches[i, h].start()

    fetch_w.wait()
    fetch_own.wait()
    inner = (z > 0) & (z < nz - 1)

    @pl.when(inner)
    def _():
        pl.semaphore_wait(barrier, GROUP + 2)

    @pl.when(jnp.logical_not(inner))
    def _():
        pl.semaphore_wait(barrier, GROUP + 1)

    w_copies, s_copies, x_copies, core_copies = {}, {}, {}, {}
    for j in (3, 1, 2):
        w_copies[j] = remote(
            wt_ref.at[:, lanes((quarter + steps[j]) * fq, fq)], w_all.at[w_rows(me), :],
            w_send.at[j], w_recv.at[j], (me + steps[j], core))
        w_copies[j].start()

    def chain(origin, way, k, j):
        rows = w_rows(origin * GROUP + quarter + steps[j])
        dev = (me + GROUP * way, core)
        return remote(w_all.at[rows, :], w_all.at[rows, :],
                      g_send.at[(1 - way) // 2, k, j], g_recv.at[origin, j], dev)

    def chain_pass(k, j):
        for side, way, onward, behind in ways:
            origin = z - way * k

            @pl.when((origin >= 0) & (origin < nz) & onward)
            def _():
                if k > 0:
                    chain(origin, -way, k, j).wait_recv()
                chain(origin, way, k, j).start()

    def chain_end(k):
        for side, way, onward, behind in ways:
            origin = z - way * k

            @pl.when((origin >= 0) & (origin < nz) & jnp.logical_not(onward))
            def _():
                for j in range(GROUP):
                    chain(origin, -way, k, j).wait_recv()

    chain_pass(0, 0)

    fetch_g.wait()
    positions = lax.broadcasted_iota(jnp.int32, (tok, 128), 0)
    factor = jnp.zeros((tok, 128), jnp.float32)
    for i in range(counts_ref.shape[1]):
        start = jnp.full((tok, 128), offsets_ref[0, i], jnp.int32)
        length = jnp.full((tok, 128), counts_ref[0, i], jnp.int32)
        inside = (positions >= start) & (positions < start + length)
        factor += jnp.where(inside, lax.rsqrt(length.astype(jnp.float32)), 0.0)
    for i in range(half // 128):
        cols = slice(i * 128, (i + 1) * 128)
        s_all[core, 0:tok, cols] = (g_ref[:, cols].astype(jnp.float32) * factor).astype(jnp.bfloat16)

    hop = tok // 2

    def s_rows(j, h):
        return ((j - 1 + h) % 2) * hop

    for h in range(2):
        for j in (1, 2):
            s_copies[j, h] = remote(
                s_all.at[core, pl.ds(s_rows(j, h), hop), :],
                s_all.at[core, pl.ds(j * tok + s_rows(j, h), hop), :],
                s_send.at[2 * j - 2 + h], s_recv.at[2 * j - 2 + h], (me + steps[j], core))
            s_copies[j, h].start()

    def to_core(j):
        core_copies[j] = remote(
            s_all.at[core, slot(j), :], s_all.at[core, slot(j), :], c_send.at[j], c_recv.at[j], (me, sib))
        core_copies[j].start()

    to_core(0)
    for j in (2, 3, 1):
        w_copies[j].wait_recv()
        chain_pass(0, j)

    for j, onto in ((1, 2), (2, 1)):
        s_copies[j, 0].wait_recv()
        s_copies[3, j - 1] = remote(
            s_all.at[core, pl.ds(j * tok + s_rows(j, 0), hop), :],
            s_all.at[core, pl.ds(3 * tok + s_rows(j, 0), hop), :],
            s_send.at[3 + j], s_recv.at[3 + j], (me + steps[onto], core))
        s_copies[3, j - 1].start()

    for i in range(nz):
        for j in (3, 1, 2):
            x_fetches[i, j].wait()
            x_copies[i, j] = remote(
                x_src.at[i, j - 1], x_all.at[i, core, slot(j), :],
                x_send.at[i, j], x_recv.at[i, j], (me + steps[j], core))
            x_copies[i, j].start()

    for j in (0, 2, 3, 1):
        chain_pass(1, j)
    for j in (1, 2):
        s_copies[j, 1].wait_recv()
        to_core(j)
    for h in range(2):
        s_copies[3, h].wait_recv()
    to_core(3)
    chain_end(1)
    for j in range(GROUP):
        core_copies[j].wait_recv()
    near = pl.ds(pl.multiple_of(upper * half, half), half)
    far = pl.ds(pl.multiple_of((1 - upper) * half, half), half)
    for j in range(GROUP):
        acc[slot(j), :] = jnp.dot(s_all[upper, slot(j), :], w_all[near, :], preferred_element_type=jnp.float32)
    for k in range(2, nz):
        for j in (0, 2, 3, 1):
            chain_pass(k, j)

    def partial_copy(t, side, h, way):
        return remote(part_out.at[t, h], part_in.at[side, t, h],
                      p_send.at[t, h], p_recv.at[side, t, h], (me + GROUP * way, core))

    def toward(t, side):
        return t > z if side == 0 else t < z

    xs_copies = {}

    def block(i):
        t = order[i]
        for j in range(1, GROUP):
            x_copies[i, j].wait_recv()
        arrived = x_all.at[i, core, pl.ds(tok, (GROUP - 1) * tok), :]
        xs_copies[i] = remote(arrived, arrived, xs_send.at[i], xs_recv.at[i], (me, sib))
        xs_copies[i].start()
        for h in range(2):
            own_fetches[i, h].wait()
        for h in (core, sib):
            if h is sib:
                xs_copies[i].wait_recv()
            part_own[t, h] = lax.dot_general(
                x_all[i, h], s_all[core], (((0,), (0,)), ((), ())), preferred_element_type=jnp.float32)
            for side, way, onward, behind in ways:
                @pl.when(toward(t, side) & jnp.logical_not(behind))
                def _():
                    part_out[t, h] = part_own[t, h].astype(jnp.bfloat16)
                    partial_copy(t, side, h, way).start()

    def forward(i, h):
        t = order[i]
        for side, way, onward, behind in ways:
            @pl.when(toward(t, side) & behind)
            def _():
                copy = partial_copy(t, side, h, way)
                copy.wait_recv()
                part_out[t, h] = (
                    part_own[t, h] + part_in[side, t, h].astype(jnp.float32)
                ).astype(jnp.bfloat16)
                copy.start()

    block(0)
    block(1)
    for k in range(2, nz):
        chain_end(k)
    o_copies = {}
    own_lanes = lanes(quarter * fq, fq)
    for j in (3, 1, 2, 0):
        product = acc[slot(j), :] + jnp.dot(
            s_all[1 - upper, slot(j), :], w_all[far, :], preferred_element_type=jnp.float32)
        if j == 0:
            dx_ref[:, own_lanes] = product.astype(jnp.bfloat16)
        else:
            dx_out[j] = product.astype(jnp.bfloat16)
            o_copies[j] = remote(
                dx_out.at[j], dx_ref.at[:, own_lanes], o_send.at[j], o_recv.at[j], (me + steps[j], core))
            o_copies[j].start()

    for h in (core, sib):
        forward(0, h)
    for i in range(2, nz):
        block(i)
    for h in (core, sib):
        for i in list(range(2, nz)) + [1]:
            forward(i, h)

    for h in (core, sib):
        for side, way, onward, behind in ways:
            @pl.when(behind)
            def _():
                partial_copy(z, side, h, -way).wait_recv()
                part_own[z, h] = part_own[z, h] + part_in[side, z, h].astype(jnp.float32)
        dw_ref[pl.ds(pl.multiple_of(h * hr, hr), hr), :] = part_own[z, h] * normalizer

    for j in (1, 2, 3):
        remote(dx_out.at[j], dx_ref.at[:, lanes((quarter + steps[j]) * fq, fq)],
               o_send.at[j], o_recv.at[j], (me + steps[j], core)).wait_recv()

    for group in (w_copies, s_copies, x_copies, o_copies, core_copies, xs_copies):
        for copy in group.values():
            copy.wait_send()
    for t in range(nz):
        for h in range(2):
            for side, way, onward, behind in ways:
                @pl.when(toward(t, side))
                def _():
                    partial_copy(t, side, h, way).wait_send()
    for k in range(nz):
        for j in range(GROUP):
            for side, way, onward, behind in ways:
                origin = z - way * k

                @pl.when((origin >= 0) & (origin < nz) & onward)
                def _():
                    chain(origin, way, k, j).wait_send()


def emit(dx_ref, dw_ref, dx_out, dw_out, sems):
    copies = [
        pltpu.make_async_copy(dx_ref, dx_out, sems.at[0]),
        pltpu.make_async_copy(dw_ref, dw_out, sems.at[1]),
    ]
    for copy in copies:
        copy.start()
    for copy in copies:
        copy.wait()


def fused(n, inputs, value_grad, value_weight, counts, offsets):
    tok, width = inputs.shape
    half = value_grad.shape[1]
    wfeat, wcols = value_weight.shape
    nz = n // GROUP
    fq = wfeat // GROUP
    hr = width // n // 2
    bf, f32, dma = jnp.bfloat16, jnp.float32, pltpu.SemaphoreType.DMA
    normalizer = 1.0 / math.sqrt(counts.shape[1] * n)
    vmem = pl.BlockSpec(memory_space=pltpu.VMEM)
    smem = pl.BlockSpec(memory_space=pltpu.SMEM)
    hbm = pl.BlockSpec(memory_space=pltpu.HBM)
    held = pl.pallas_call(
        functools.partial(kernel, n, normalizer),
        out_shape=(pltpu.VMEM((tok, wfeat), bf), pltpu.VMEM((2 * hr, half), f32)),
        in_specs=[smem] * 2 + [hbm] * 3,
        out_specs=(vmem, vmem),
        scratch_shapes=[
            pltpu.VMEM((tok, half), bf),
            pltpu.VMEM((wcols, wfeat), bf),
            pltpu.VMEM((nz, GROUP - 1, tok, hr), bf),
            pltpu.VMEM((2, GROUP * tok, half), bf),
            pltpu.VMEM((nz, 2, GROUP * tok, hr), bf),
            pltpu.VMEM((n * wcols, fq), bf),
            pltpu.VMEM((GROUP * tok, fq), f32),
            pltpu.VMEM((nz, 2, hr, half), f32),
            pltpu.VMEM((nz, 2, hr, half), bf),
            pltpu.VMEM((2, nz, 2, hr, half), bf),
            pltpu.VMEM((GROUP, tok, fq), bf),
            dma((3,)), dma((nz, GROUP - 1)), dma((nz, 2)),
            dma((GROUP,)), dma((GROUP,)),
            dma((6,)), dma((6,)),
            dma((GROUP,)), dma((GROUP,)),
            dma((nz, GROUP)), dma((nz, GROUP)),
            dma((nz,)), dma((nz,)),
            dma((2, nz, GROUP)), dma((nz, GROUP)),
            dma((nz, 2)), dma((2, nz, 2)),
            dma((GROUP,)), dma((GROUP,)),
        ],
        compiler_params=pltpu.CompilerParams(
            collective_id=0, has_side_effects=True, vmem_limit_bytes=VMEM_ROOM
        ),
    )(counts, offsets, inputs, value_grad, value_weight.T)
    return pl.pallas_call(
        emit,
        out_shape=(
            jax.ShapeDtypeStruct((tok, wfeat), bf),
            jax.ShapeDtypeStruct((2 * hr, half), f32),
        ),
        in_specs=[vmem] * 2,
        out_specs=(hbm, hbm),
        scratch_shapes=[dma((2,))],
    )(*[pltpu.with_memory_space_constraint(part, pltpu.VMEM) for part in held])


def solution(mesh):
    n, tp = mesh.shape["fsdp"], mesh.shape["tp"]

    def local(inputs, value_grad, value_weight, counts, offsets):
        hr = inputs.shape[1] // n // 2
        fits = tp == 2 and n % (2 * GROUP) == 0 and n > 2 * GROUP and hr % 128 == 0
        fits = fits and value_weight.shape[1] % 16 == 0 and inputs.shape[0] % 32 == 0
        if fits:
            return fused(n, inputs, value_grad, value_weight, counts, offsets)
        return general(inputs, value_grad, value_weight, counts, offsets)

    in_specs = (P("fsdp", None), P("fsdp", "tp"), P("tp", "fsdp"), P("fsdp", None), P("fsdp", None))
    out_specs = (P("fsdp", "tp"), P("fsdp", "tp"))
    return jax.shard_map(local, mesh=mesh, in_specs=in_specs, out_specs=out_specs, check_vma=False)
```

```python
import functools
import math

import jax
import jax.numpy as jnp
from jax import lax
from jax.experimental import pallas as pl
from jax.experimental.pallas import tpu as pltpu
from jax.sharding import PartitionSpec as P

MESH = pl.DeviceIdType.MESH
GROUP = 4
LANES = 4
VMEM_ROOM = 54 * 2**20


def scale_rows(value_grad, counts, offsets):
    positions = jnp.arange(value_grad.shape[0], dtype=jnp.int32)[:, None]
    starts = offsets[0][None, :]
    lengths = counts[0][None, :]
    inside = (positions >= starts) & (positions < starts + lengths)
    inverse_root = lax.rsqrt(lengths.astype(jnp.float32))
    row_factor = jnp.sum(jnp.where(inside, inverse_root, jnp.zeros_like(inverse_root)), axis=1)
    return (value_grad.astype(jnp.float32) * row_factor[:, None]).astype(jnp.bfloat16)


def general(inputs, value_grad, value_weight, counts, offsets):
    tok_rows = inputs.shape[0]
    row_block = min(128, tok_rows)
    scaled = scale_rows(value_grad, counts, offsets)
    live_end = jnp.max(offsets[0] + counts[0])
    live_blocks = (live_end + row_block - 1) // row_block
    scaled_all = lax.all_gather(scaled, "tp", axis=1, tiled=True)
    empty_inputs = jnp.zeros((tok_rows, value_weight.shape[0]), jnp.float32)
    piece = lax.all_gather(value_weight, "fsdp", axis=1, tiled=True)

    def add_add_block(block_index, partial_value):
        lower = lax.dynamic_slice_in_dim(scaled_all, block_index * row_block, row_block, 0)
        before = lax.dynamic_slice_in_dim(partial_value, block_index * row_block, row_block, 0)
        product = lax.dot_general(
            lower, piece, (((1,), (1,)), ((), ())), preferred_element_type=jnp.float32
        )
        return lax.dynamic_update_slice_in_dim(
            partial_value, before + product, block_index * row_block, 0
        )

    result = lax.fori_loop(0, live_blocks, add_add_block, empty_inputs)
    input_grad = result.astype(jnp.bfloat16)
    normalizer = 1.0 / math.sqrt(counts.shape[1] * lax.axis_size("fsdp"))
    empty = jnp.zeros((inputs.shape[1], scaled.shape[1]), jnp.float32)

    def weight_add_block(block_index, partial_value):
        feature_rows = lax.dynamic_slice_in_dim(inputs, block_index * row_block, row_block, 0)
        grad_rows = lax.dynamic_slice_in_dim(scaled, block_index * row_block, row_block, 0)
        return partial_value + lax.dot_general(
            feature_rows, grad_rows, (((0,), (0,)), ((), ())), preferred_element_type=jnp.float32
        )

    result = lax.fori_loop(0, live_blocks, weight_add_block, empty)
    summed = lax.psum_scatter(result, "fsdp", scatter_dimension=0, tiled=True)
    return (input_grad, summed * normalizer)


def kernel(
    n, normalizer, counts_hbm, offsets_hbm, x_hbm, g_hbm, wt_hbm, dx_ref, dw_ref,
    counts_ref, offsets_ref, g_ref, wt_ref, x_src, s_all, x_all, w_all, acc, part_own, part_out, part_in,
    dx_out, local_sem, w_send, w_recv, s_send, s_recv, c_send, c_recv, x_send, x_recv,
    xs_send, xs_recv, g_send, g_recv, p_send, p_recv, o_send, o_recv,
):
    nz = n // GROUP
    me = lax.axis_index("fsdp")
    core = lax.axis_index("tp")
    sib = 1 - core
    z = me // GROUP
    quarter = me % GROUP
    dx = 1 - 2 * (me % 2)
    dy = 2 - 4 * ((me // 2) % 2)
    steps = (0, dx, dy, dx + dy)
    tok, half = g_ref.shape
    wcols = wt_ref.shape[0]
    fq = w_all.shape[1]
    hr = x_src.shape[3]
    zrows = GROUP * wcols
    lane_rows = part_out.shape[1] // LANES
    upper = (2 * z) // nz
    order = [a + upper * (nz - 1 - 2 * a) for a in
             list(range(nz - 1, nz // 2 - 1, -1)) + list(range(nz // 2))]
    ways = ((0, 1, z < nz - 1, z > 0), (1, -1, z > 0, z < nz - 1))
    inner = (z > 0) & (z < nz - 1)

    barrier = pltpu.get_barrier_semaphore()
    for j in range(1, GROUP):
        pl.semaphore_signal(barrier, inc=1, device_id=(me + steps[j], core), device_id_type=MESH)
    pl.semaphore_signal(barrier, inc=1, device_id=(me, sib), device_id_type=MESH)
    for side, way, onward, behind in ways:
        @pl.when(onward)
        def _():
            pl.semaphore_signal(barrier, inc=1, device_id=(me + GROUP * way, core), device_id_type=MESH)

    def remote(src, dst, send, recv, dev):
        return pltpu.make_async_remote_copy(
            src_ref=src, dst_ref=dst, send_sem=send, recv_sem=recv,
            device_id=dev, device_id_type=MESH,
        )

    def sent(ref, sem):
        remote(ref, ref, sem, sem, (me, sib)).wait_send()

    def received(ref, sem):
        remote(ref, ref, sem, sem, (me, sib)).wait_recv()

    def w_rows(f):
        return pl.ds(pl.multiple_of(f * wcols, wcols), wcols)

    def lanes(start, size):
        return pl.ds(pl.multiple_of(start, 128), size)

    def slot(j):
        return pl.ds(j * tok, tok)

    def x_lanes(i, q, h):
        return lanes(((order[i] * GROUP + q) * 2 + h) * hr, hr)

    others = pl.ds(tok, (GROUP - 1) * tok)
    mine = lanes(core * hr, hr)

    fetch_w = pltpu.make_async_copy(wt_hbm, wt_ref, local_sem.at[0])
    fetch_own = pltpu.make_async_copy(
        wt_hbm.at[:, lanes(quarter * fq, fq)], w_all.at[w_rows(me), :], local_sem.at[1])
    fetch_g = pltpu.make_async_copy(g_hbm, g_ref, local_sem.at[2])
    fetch_counts = pltpu.make_async_copy(counts_hbm, counts_ref, local_sem.at[3])
    fetch_offsets = pltpu.make_async_copy(offsets_hbm, offsets_ref, local_sem.at[4])
    for fetch in (fetch_w, fetch_own, fetch_g, fetch_counts, fetch_offsets):
        fetch.start()
    for i in range(nz):
        for j in (3, 1, 2):
            pltpu.make_async_copy(
                x_hbm.at[:, x_lanes(i, quarter + steps[j], core)], x_src.at[i, j - 1], local_sem.at[5]).start()
    for i in range(nz):
        block_lanes = lanes((order[i] * GROUP + quarter) * 2 * hr, 2 * hr)
        pltpu.make_async_copy(x_hbm.at[:, block_lanes], x_all.at[i, slot(0), :], local_sem.at[6]).start()

    fetch_w.wait()
    fetch_own.wait()

    @pl.when(inner)
    def _():
        pl.semaphore_wait(barrier, GROUP + 2)

    @pl.when(jnp.logical_not(inner))
    def _():
        pl.semaphore_wait(barrier, GROUP + 1)

    for j in (3, 1, 2):
        remote(wt_ref.at[:, lanes((quarter + steps[j]) * fq, fq)], w_all.at[w_rows(me), :],
               w_send, w_recv.at[j - 1], (me + steps[j], core)).start()

    def chain(origin, way, j):
        rows = w_rows(origin * GROUP + quarter + steps[j])
        return remote(w_all.at[rows, :], w_all.at[rows, :],
                      g_send.at[(1 - way) // 2], g_recv.at[origin, j], (me + GROUP * way, core))

    def chain_pass(k, j):
        for side, way, onward, behind in ways:
            origin = z - way * k

            @pl.when((origin >= 0) & (origin < nz) & onward)
            def _():
                if k > 0:
                    chain(origin, -way, j).wait_recv()
                chain(origin, way, j).start()

    def chain_end(k):
        for side, way, onward, behind in ways:
            origin = z - way * k

            @pl.when((origin >= 0) & (origin < nz) & jnp.logical_not(onward))
            def _():
                for j in range(GROUP):
                    chain(origin, -way, j).wait_recv()

    chain_pass(0, 0)

    for fetch in (fetch_g, fetch_counts, fetch_offsets):
        fetch.wait()
    positions = lax.broadcasted_iota(jnp.int32, (tok, 128), 0)
    factor = jnp.zeros((tok, 128), jnp.float32)
    for i in range(counts_ref.shape[1]):
        start = jnp.full((tok, 128), offsets_ref[0, i], jnp.int32)
        length = jnp.full((tok, 128), counts_ref[0, i], jnp.int32)
        inside = (positions >= start) & (positions < start + length)
        factor += jnp.where(inside, lax.rsqrt(length.astype(jnp.float32)), 0.0)
    for i in range(half // 128):
        cols = slice(i * 128, (i + 1) * 128)
        s_all[core, 0:tok, cols] = (g_ref[:, cols].astype(jnp.float32) * factor).astype(jnp.bfloat16)

    hop = tok // 2

    def s_send_rows(j, src_slot, dst_slot, h, sem, onto):
        first = ((j - 1 + h) % 2) * hop
        remote(s_all.at[core, pl.ds(src_slot * tok + first, hop), :],
               s_all.at[core, pl.ds(dst_slot * tok + first, hop), :],
               s_send, s_recv.at[sem], (me + steps[onto], core)).start()

    for h in range(2):
        for j in (1, 2):
            s_send_rows(j, 0, j, h, 2 if h else j - 1, j)

    def to_core(first, count):
        rows = pl.ds(first * tok, count * tok)
        remote(s_all.at[core, rows, :], s_all.at[core, rows, :], c_send, c_recv, (me, sib)).start()

    to_core(0, 1)

    def x_start(i):
        for j in (3, 1, 2):
            remote(x_src.at[i, j - 1], x_all.at[i, slot(j), mine],
                   x_send, x_recv.at[i], (me + steps[j], core)).start()

    pltpu.make_async_copy(x_src, x_src, local_sem.at[5]).wait()
    x_start(0)
    for j in (2, 3, 1):
        received(w_all.at[w_rows(me), :], w_recv.at[j - 1])
        chain_pass(0, j)
    for j, onto in ((1, 2), (2, 1)):
        received(s_all.at[core, pl.ds(0, hop), :], s_recv.at[j - 1])
        s_send_rows(j, j, 3, 0, 3, onto)
    for i in range(1, nz):
        x_start(i)
    for j in (0, 2, 3, 1):
        chain_pass(1, j)
    received(s_all.at[core, pl.ds(0, 2 * hop), :], s_recv.at[2])
    to_core(1, 2)

    def partial_copy(t, side, lane, way, target):
        place = t if side == 0 else jnp.where(t == target, nz, t)
        rows = pl.ds(lane * lane_rows, lane_rows)
        return remote(part_out.at[t, rows, :], part_in.at[place, rows, :],
                      p_send, p_recv.at[place, lane], (me + GROUP * way, core))

    def toward(t, side):
        return t > z if side == 0 else t < z

    def x_swap(i):
        received(x_all.at[i, others, mine], x_recv.at[i])
        remote(x_all.at[i, others, mine], x_all.at[i, others, mine], xs_send, xs_recv.at[i], (me, sib)).start()

    def contract(i, rows):
        return lax.dot_general(x_all[i, rows, :], s_all[core, rows, :], (((0,), (0,)), ((), ())),
                               preferred_element_type=jnp.float32)

    def launch(i):
        t = order[i]
        for side, way, onward, behind in ways:
            @pl.when(toward(t, side) & jnp.logical_not(behind))
            def _():
                for lane in range(LANES):
                    rows = pl.ds(lane * lane_rows, lane_rows)
                    part_out[t, rows, :] = part_own[t, rows, :].astype(jnp.bfloat16)
                    partial_copy(t, side, lane, way, z + way).start()

    def block(i):
        x_swap(i)
        received(x_all.at[i, others, mine], xs_recv.at[i])
        part_own[order[i]] = contract(i, pl.ds(0, GROUP * tok))
        launch(i)

    def forward(i, lane):
        t = order[i]
        rows = pl.ds(lane * lane_rows, lane_rows)
        for side, way, onward, behind in ways:
            @pl.when(toward(t, side) & behind)
            def _():
                partial_copy(t, side, lane, -way, z).wait_recv()
                part_out[t, rows, :] = (
                    part_own[t, rows, :] + part_in[t, rows, :].astype(jnp.float32)
                ).astype(jnp.bfloat16)
                partial_copy(t, side, lane, way, z + way).start()

    pltpu.make_async_copy(x_all.at[:, slot(0), :], x_all.at[:, slot(0), :], local_sem.at[6]).wait()
    x_swap(0)
    received(x_all.at[0, others, mine], xs_recv.at[0])
    part_own[order[0]] = contract(0, pl.ds(0, (GROUP - 1) * tok))
    for k in range(2, nz):
        for j in (0, 2, 3, 1):
            chain_pass(k, j)
    received(s_all.at[core, pl.ds(0, 2 * hop), :], s_recv.at[3])
    to_core(3, 1)
    part_own[order[0]] = part_own[order[0]] + contract(0, slot(GROUP - 1))
    launch(0)

    chain_end(1)
    received(s_all.at[core], c_recv)
    near = pl.ds(pl.multiple_of(upper * half, half), half)
    far = pl.ds(pl.multiple_of((1 - upper) * half, half), half)
    for j in range(GROUP):
        acc[slot(j), :] = jnp.dot(s_all[upper, slot(j), :], w_all[near, :], preferred_element_type=jnp.float32)
    block(1)
    for k in range(2, nz):
        chain_end(k)
    own_lanes = lanes(quarter * fq, fq)
    first = jnp.where(quarter == 1, 1, GROUP - 1)
    for j, step in ((first, jnp.where(quarter == 1, steps[1], steps[3])),
                    (GROUP - first, jnp.where(quarter == 1, steps[3], steps[1])),
                    (2, steps[2]), (0, None)):
        rows = pl.ds(pl.multiple_of(j * tok, tok), tok)
        product = acc[rows, :] + jnp.dot(
            s_all[1 - upper, rows, :], w_all[far, :], preferred_element_type=jnp.float32)
        if step is None:
            dx_ref[:, own_lanes] = product.astype(jnp.bfloat16)
        else:
            dx_out[j - 1] = product.astype(jnp.bfloat16)
            remote(dx_out.at[j - 1], dx_ref.at[:, own_lanes], o_send, o_recv, (me + step, core)).start()

    for lane in range(LANES):
        forward(0, lane)
    for i in range(2, nz):
        block(i)
    for lane in range(LANES):
        for i in list(range(2, nz)) + [1]:
            forward(i, lane)

    for lane in range(LANES):
        rows = pl.ds(lane * lane_rows, lane_rows)
        for side, way, onward, behind in ways:
            @pl.when(behind)
            def _():
                partial_copy(z, side, lane, -way, z).wait_recv()
                place = z if side == 0 else nz
                part_own[z, rows, :] = part_own[z, rows, :] + part_in[place, rows, :].astype(jnp.float32)
        dw_ref[rows, :] = part_own[z, rows, :] * normalizer

    received(dx_out, o_recv)

    sent(w_all.at[pl.ds(0, (GROUP - 1) * wcols), :], w_send)
    sent(s_all.at[0, others, :], s_send)
    sent(s_all.at[0], c_send)
    sent(x_src, x_send)
    sent(x_all.at[:, others, mine], xs_send)
    sent(dx_out, o_send)
    sent(part_out.at[pl.ds(0, nz - 1)], p_send)
    for level in range(nz):
        @pl.when(z == level)
        def _():
            if level < nz - 1:
                sent(w_all.at[pl.ds(0, (level + 1) * zrows), :], g_send.at[0])
            if level > 0:
                sent(w_all.at[pl.ds(0, (nz - level) * zrows), :], g_send.at[1])


def emit(dx_ref, dw_ref, dx_out, dw_out, sems):
    copies = [
        pltpu.make_async_copy(dx_ref, dx_out, sems.at[0]),
        pltpu.make_async_copy(dw_ref, dw_out, sems.at[1]),
    ]
    for copy in copies:
        copy.start()
    for copy in copies:
        copy.wait()


def fused(n, inputs, value_grad, value_weight, counts, offsets):
    tok, width = inputs.shape
    half = value_grad.shape[1]
    wfeat, wcols = value_weight.shape
    nz = n // GROUP
    fq = wfeat // GROUP
    hr = width // n // 2
    bf, f32, dma = jnp.bfloat16, jnp.float32, pltpu.SemaphoreType.DMA
    normalizer = 1.0 / math.sqrt(counts.shape[1] * n)
    vmem = pl.BlockSpec(memory_space=pltpu.VMEM)
    hbm = pl.BlockSpec(memory_space=pltpu.HBM)
    held = pl.pallas_call(
        functools.partial(kernel, n, normalizer),
        out_shape=(pltpu.VMEM((tok, wfeat), bf), pltpu.VMEM((2 * hr, half), f32)),
        in_specs=[hbm] * 5,
        out_specs=(vmem, vmem),
        scratch_shapes=[
            pltpu.SMEM(counts.shape, jnp.int32),
            pltpu.SMEM(offsets.shape, jnp.int32),
            pltpu.VMEM((tok, half), bf),
            pltpu.VMEM((wcols, wfeat), bf),
            pltpu.VMEM((nz, GROUP - 1, tok, hr), bf),
            pltpu.VMEM((2, GROUP * tok, half), bf),
            pltpu.VMEM((nz, GROUP * tok, 2 * hr), bf),
            pltpu.VMEM((n * wcols, fq), bf),
            pltpu.VMEM((GROUP * tok, fq), f32),
            pltpu.VMEM((nz, 2 * hr, half), f32),
            pltpu.VMEM((nz, 2 * hr, half), bf),
            pltpu.VMEM((nz + 1, 2 * hr, half), bf),
            pltpu.VMEM((GROUP - 1, tok, fq), bf),
            dma((7,)),
            dma, dma((GROUP - 1,)),
            dma, dma((4,)),
            dma, dma,
            dma, dma((nz,)),
            dma, dma((nz,)),
            dma((2,)), dma((nz, GROUP)),
            dma, dma((nz + 1, LANES)),
            dma, dma,
        ],
        compiler_params=pltpu.CompilerParams(
            collective_id=0, has_side_effects=True, vmem_limit_bytes=VMEM_ROOM
        ),
    )(counts, offsets, inputs, value_grad, value_weight.T)
    return pl.pallas_call(
        emit,
        out_shape=(
            jax.ShapeDtypeStruct((tok, wfeat), bf),
            jax.ShapeDtypeStruct((2 * hr, half), f32),
        ),
        in_specs=[vmem] * 2,
        out_specs=(hbm, hbm),
        scratch_shapes=[dma((2,))],
    )(*[pltpu.with_memory_space_constraint(part, pltpu.VMEM) for part in held])


def solution(mesh):
    n, tp = mesh.shape["fsdp"], mesh.shape["tp"]

    def local(inputs, value_grad, value_weight, counts, offsets):
        hr = inputs.shape[1] // n // 2
        fits = tp == 2 and n % (2 * GROUP) == 0 and n > 2 * GROUP and hr % 128 == 0
        fits = fits and value_weight.shape[1] % 16 == 0 and inputs.shape[0] % 32 == 0
        if fits:
            return fused(n, inputs, value_grad, value_weight, counts, offsets)
        return general(inputs, value_grad, value_weight, counts, offsets)

    in_specs = (P("fsdp", None), P("fsdp", "tp"), P("tp", "fsdp"), P("fsdp", None), P("fsdp", None))
    out_specs = (P("fsdp", "tp"), P("fsdp", "tp"))
    return jax.shard_map(local, mesh=mesh, in_specs=in_specs, out_specs=out_specs, check_vma=False)
```

```python
import functools
import math

import jax
import jax.numpy as jnp
from jax import lax
from jax.experimental import pallas as pl
from jax.experimental.pallas import tpu as pltpu
from jax.sharding import PartitionSpec as P

MESH = pl.DeviceIdType.MESH
GROUP = 4
LANES = 4
CHUNKS = 8
VMEM_ROOM = 54 * 2**20


def scale_rows(value_grad, counts, offsets):
    positions = jnp.arange(value_grad.shape[0], dtype=jnp.int32)[:, None]
    starts = offsets[0][None, :]
    lengths = counts[0][None, :]
    inside = (positions >= starts) & (positions < starts + lengths)
    inverse_root = lax.rsqrt(lengths.astype(jnp.float32))
    row_factor = jnp.sum(jnp.where(inside, inverse_root, jnp.zeros_like(inverse_root)), axis=1)
    return (value_grad.astype(jnp.float32) * row_factor[:, None]).astype(jnp.bfloat16)


def general(inputs, value_grad, value_weight, counts, offsets):
    tok_rows = inputs.shape[0]
    row_block = min(128, tok_rows)
    scaled = scale_rows(value_grad, counts, offsets)
    live_end = jnp.max(offsets[0] + counts[0])
    live_blocks = (live_end + row_block - 1) // row_block
    scaled_all = lax.all_gather(scaled, "tp", axis=1, tiled=True)
    empty_inputs = jnp.zeros((tok_rows, value_weight.shape[0]), jnp.float32)
    piece = lax.all_gather(value_weight, "fsdp", axis=1, tiled=True)

    def add_add_block(block_index, partial_value):
        lower = lax.dynamic_slice_in_dim(scaled_all, block_index * row_block, row_block, 0)
        before = lax.dynamic_slice_in_dim(partial_value, block_index * row_block, row_block, 0)
        product = lax.dot_general(
            lower, piece, (((1,), (1,)), ((), ())), preferred_element_type=jnp.float32
        )
        return lax.dynamic_update_slice_in_dim(
            partial_value, before + product, block_index * row_block, 0
        )

    result = lax.fori_loop(0, live_blocks, add_add_block, empty_inputs)
    input_grad = result.astype(jnp.bfloat16)
    normalizer = 1.0 / math.sqrt(counts.shape[1] * lax.axis_size("fsdp"))
    empty = jnp.zeros((inputs.shape[1], scaled.shape[1]), jnp.float32)

    def weight_add_block(block_index, partial_value):
        feature_rows = lax.dynamic_slice_in_dim(inputs, block_index * row_block, row_block, 0)
        grad_rows = lax.dynamic_slice_in_dim(scaled, block_index * row_block, row_block, 0)
        return partial_value + lax.dot_general(
            feature_rows, grad_rows, (((0,), (0,)), ((), ())), preferred_element_type=jnp.float32
        )

    result = lax.fori_loop(0, live_blocks, weight_add_block, empty)
    summed = lax.psum_scatter(result, "fsdp", scatter_dimension=0, tiled=True)
    return (input_grad, summed * normalizer)


def kernel(
    n, normalizer, counts_hbm, offsets_hbm, x_hbm, g_hbm, wt_hbm, dx_ref, dw_ref,
    counts_ref, offsets_ref, g_ref, wt_ref, x_src, s_all, x_all, w_all, acc, part_own, part_out, part_in,
    dx_out, local_sem, w_send, w_recv, s_send, s_recv, c_send, c_recv, x_send, x_recv,
    xs_send, xs_recv, g_send, g_recv, p_send, p_recv, o_send, o_recv, ready,
):
    nz = n // GROUP
    me = lax.axis_index("fsdp")
    core = lax.axis_index("tp")
    sib = 1 - core
    z = me // GROUP
    quarter = me % GROUP
    dx = 1 - 2 * (me % 2)
    dy = 2 - 4 * ((me // 2) % 2)
    steps = (0, dx, dy, dx + dy)
    tok, half = g_ref.shape
    wcols = wt_ref.shape[0]
    fq = w_all.shape[1]
    hr = x_src.shape[3]
    zrows = GROUP * wcols
    lane_rows = part_out.shape[1] // LANES
    upper = (2 * z) // nz
    order = [a + upper * (nz - 1 - 2 * a) for a in
             list(range(nz - 1, nz // 2 - 1, -1)) + list(range(nz // 2))]
    ways = ((0, 1, z < nz - 1, z > 0), (1, -1, z > 0, z < nz - 1))
    barrier = pltpu.get_barrier_semaphore()
    for j in range(1, GROUP):
        pl.semaphore_signal(barrier, inc=1, device_id=(me + steps[j], core), device_id_type=MESH)
    pl.semaphore_signal(barrier, inc=1, device_id=(me, sib), device_id_type=MESH)

    @pl.when(z < nz - 1)
    def _():
        pl.semaphore_signal(barrier, inc=1, device_id=(me + GROUP, core), device_id_type=MESH)

    def remote(src, dst, send, recv, dev):
        return pltpu.make_async_remote_copy(
            src_ref=src, dst_ref=dst, send_sem=send, recv_sem=recv,
            device_id=dev, device_id_type=MESH,
        )

    def sent(ref, sem):
        remote(ref, ref, sem, sem, (me, sib)).wait_send()

    def received(ref, sem):
        remote(ref, ref, sem, sem, (me, sib)).wait_recv()

    def w_rows(f):
        return pl.ds(pl.multiple_of(f * wcols, wcols), wcols)

    def lanes(start, size):
        return pl.ds(pl.multiple_of(start, 128), size)

    def slot(j):
        return pl.ds(j * tok, tok)

    def x_lanes(i, q, h):
        return lanes(((order[i] * GROUP + q) * 2 + h) * hr, hr)

    others = pl.ds(tok, (GROUP - 1) * tok)
    mine = lanes(core * hr, hr)

    fetch_w = pltpu.make_async_copy(wt_hbm, wt_ref, local_sem.at[0])
    fetch_own = pltpu.make_async_copy(
        wt_hbm.at[:, lanes(quarter * fq, fq)], w_all.at[w_rows(me), :], local_sem.at[1])
    fetch_g = pltpu.make_async_copy(g_hbm, g_ref, local_sem.at[2])
    fetch_counts = pltpu.make_async_copy(counts_hbm, counts_ref, local_sem.at[3])
    fetch_offsets = pltpu.make_async_copy(offsets_hbm, offsets_ref, local_sem.at[4])
    for fetch in (fetch_w, fetch_own, fetch_g, fetch_counts, fetch_offsets):
        fetch.start()
    for i in range(nz):
        for j in (3, 1, 2):
            pltpu.make_async_copy(
                x_hbm.at[:, x_lanes(i, quarter + steps[j], core)], x_src.at[i, j - 1], local_sem.at[5]).start()
    for i in range(nz):
        block_lanes = lanes((order[i] * GROUP + quarter) * 2 * hr, 2 * hr)
        pltpu.make_async_copy(x_hbm.at[:, block_lanes], x_all.at[i, slot(0), :], local_sem.at[6]).start()

    fetch_w.wait()

    @pl.when(z > 0)
    def _():
        pl.semaphore_wait(barrier, GROUP + 1)
        pl.semaphore_signal(ready, inc=1, device_id=(me - GROUP, core), device_id_type=MESH)

    @pl.when(z == 0)
    def _():
        pl.semaphore_wait(barrier, GROUP)

    for j in (3, 1, 2):
        remote(wt_ref.at[:, lanes((quarter + steps[j]) * fq, fq)], w_all.at[w_rows(me), :],
               w_send, w_recv.at[j - 1], (me + steps[j], core)).start()

    def chain(origin, way, j):
        rows = w_rows(origin * GROUP + quarter + steps[j])
        return remote(w_all.at[rows, :], w_all.at[rows, :],
                      g_send.at[(1 - way) // 2], g_recv.at[origin, j], (me + GROUP * way, core))

    def chain_pass(k, j):
        for side, way, onward, behind in ways:
            origin = z - way * k

            @pl.when((origin >= 0) & (origin < nz) & onward)
            def _():
                if k > 0:
                    chain(origin, -way, j).wait_recv()
                chain(origin, way, j).start()

    def chain_end(k):
        for side, way, onward, behind in ways:
            origin = z - way * k

            @pl.when((origin >= 0) & (origin < nz) & jnp.logical_not(onward))
            def _():
                for j in range(GROUP):
                    chain(origin, -way, j).wait_recv()

    fetch_own.wait()

    @pl.when(z > 0)
    def _():
        chain(z, -1, 0).start()

    for fetch in (fetch_g, fetch_counts, fetch_offsets):
        fetch.wait()
    positions = lax.broadcasted_iota(jnp.int32, (tok, 128), 0)
    factor = jnp.zeros((tok, 128), jnp.float32)
    for i in range(counts_ref.shape[1]):
        start = jnp.full((tok, 128), offsets_ref[0, i], jnp.int32)
        length = jnp.full((tok, 128), counts_ref[0, i], jnp.int32)
        inside = (positions >= start) & (positions < start + length)
        factor += jnp.where(inside, lax.rsqrt(length.astype(jnp.float32)), 0.0)
    for i in range(half // 128):
        cols = slice(i * 128, (i + 1) * 128)
        s_all[core, 0:tok, cols] = (g_ref[:, cols].astype(jnp.float32) * factor).astype(jnp.bfloat16)

    hop = tok // 2

    def s_send_rows(j, src_slot, dst_slot, h, sem, onto):
        first = ((j - 1 + h) % 2) * hop
        remote(s_all.at[core, pl.ds(src_slot * tok + first, hop), :],
               s_all.at[core, pl.ds(dst_slot * tok + first, hop), :],
               s_send, s_recv.at[sem], (me + steps[onto], core)).start()

    for h in range(2):
        for j in (1, 2):
            s_send_rows(j, 0, j, h, 2 if h else j - 1, j)

    def to_core(first, count):
        rows = pl.ds(first * tok, count * tok)
        remote(s_all.at[core, rows, :], s_all.at[core, rows, :], c_send, c_recv, (me, sib)).start()

    to_core(0, 1)

    def x_start(i):
        for j in (3, 1, 2):
            remote(x_src.at[i, j - 1], x_all.at[i, slot(j), mine],
                   x_send, x_recv.at[i], (me + steps[j], core)).start()

    pltpu.make_async_copy(x_src, x_src, local_sem.at[5]).wait()
    x_start(0)

    @pl.when(z < nz - 1)
    def _():
        pl.semaphore_wait(ready, 1)
        chain(z, 1, 0).start()

    for j in (2, 3, 1):
        received(w_all.at[w_rows(me), :], w_recv.at[j - 1])
        chain_pass(0, j)
    for j, onto in ((1, 2), (2, 1)):
        received(s_all.at[core, pl.ds(0, hop), :], s_recv.at[j - 1])
        s_send_rows(j, j, 3, 0, 3, onto)
    for i in range(1, nz):
        x_start(i)
    for j in (0, 2, 3, 1):
        chain_pass(1, j)
    received(s_all.at[core, pl.ds(0, 2 * hop), :], s_recv.at[2])
    to_core(1, 2)

    def partial_copy(t, side, lane, way, target):
        place = t if side == 0 else jnp.where(t == target, nz, t)
        rows = pl.ds(lane * lane_rows, lane_rows)
        return remote(part_out.at[t, rows, :], part_in.at[place, rows, :],
                      p_send, p_recv.at[place, lane], (me + GROUP * way, core))

    def toward(t, side):
        return t > z if side == 0 else t < z

    def x_swap(i):
        received(x_all.at[i, others, mine], x_recv.at[i])
        remote(x_all.at[i, others, mine], x_all.at[i, others, mine], xs_send, xs_recv.at[i], (me, sib)).start()

    def contract(i, rows):
        return lax.dot_general(x_all[i, rows, :], s_all[core, rows, :], (((0,), (0,)), ((), ())),
                               preferred_element_type=jnp.float32)

    def launch(i):
        t = order[i]
        for side, way, onward, behind in ways:
            @pl.when(toward(t, side) & jnp.logical_not(behind))
            def _():
                for lane in range(LANES):
                    rows = pl.ds(lane * lane_rows, lane_rows)
                    part_out[t, rows, :] = part_own[t, rows, :].astype(jnp.bfloat16)
                    partial_copy(t, side, lane, way, z + way).start()

    def block(i):
        x_swap(i)
        received(x_all.at[i, others, mine], xs_recv.at[i])
        part_own[order[i]] = contract(i, pl.ds(0, GROUP * tok))
        launch(i)

    def forward(i, lane):
        t = order[i]
        rows = pl.ds(lane * lane_rows, lane_rows)
        for side, way, onward, behind in ways:
            @pl.when(toward(t, side) & behind)
            def _():
                partial_copy(t, side, lane, -way, z).wait_recv()
                part_out[t, rows, :] = (
                    part_own[t, rows, :] + part_in[t, rows, :].astype(jnp.float32)
                ).astype(jnp.bfloat16)
                partial_copy(t, side, lane, way, z + way).start()

    pltpu.make_async_copy(x_all.at[:, slot(0), :], x_all.at[:, slot(0), :], local_sem.at[6]).wait()
    x_swap(0)
    for k in range(2, nz):
        for j in (0, 2, 3, 1):
            chain_pass(k, j)
    received(x_all.at[0, others, mine], xs_recv.at[0])
    part_own[order[0]] = contract(0, pl.ds(0, (GROUP - 1) * tok))
    received(s_all.at[core, pl.ds(0, 2 * hop), :], s_recv.at[3])
    to_core(3, 1)
    part_own[order[0]] = part_own[order[0]] + contract(0, slot(GROUP - 1))
    launch(0)

    chain_end(1)
    received(s_all.at[core], c_recv)
    near = pl.ds(pl.multiple_of(upper * half, half), half)
    far = pl.ds(pl.multiple_of((1 - upper) * half, half), half)
    for j in range(GROUP):
        acc[slot(j), :] = jnp.dot(s_all[upper, slot(j), :], w_all[near, :], preferred_element_type=jnp.float32)

    own_lanes = lanes(quarter * fq, fq)
    first = jnp.where(quarter == 1, 1, GROUP - 1)

    def give():
        for k in range(2, nz):
            chain_end(k)
        for j, step in ((first, jnp.where(quarter == 1, steps[1], steps[3])),
                        (2, steps[2]),
                        (GROUP - first, jnp.where(quarter == 1, steps[3], steps[1])), (0, None)):
            rows = pl.ds(pl.multiple_of(j * tok, tok), tok)
            product = acc[rows, :] + jnp.dot(
                s_all[1 - upper, rows, :], w_all[far, :], preferred_element_type=jnp.float32)
            if step is None:
                dx_ref[:, own_lanes] = product.astype(jnp.bfloat16)
            else:
                dx_out[j - 1] = product.astype(jnp.bfloat16)
                remote(dx_out.at[j - 1], dx_ref.at[:, own_lanes], o_send, o_recv, (me + step, core)).start()

    between = (z > 0) & (z < nz - 1)

    @pl.when(between & (core == 0))
    def _():
        give()

    for lane in range(LANES):
        forward(0, lane)
    block(1)

    @pl.when(jnp.logical_not(between))
    def _():
        give()

    block(2)

    @pl.when(between & (core == 1))
    def _():
        give()

    for lane in range(LANES):
        forward(2, lane)
        forward(1, lane)
    for i in range(3, nz):
        block(i)
        for lane in range(LANES):
            forward(i, lane)

    for lane in range(LANES):
        rows = pl.ds(lane * lane_rows, lane_rows)
        for side, way, onward, behind in ways:
            @pl.when(behind)
            def _():
                partial_copy(z, side, lane, -way, z).wait_recv()
                place = z if side == 0 else nz
                part_own[z, rows, :] = part_own[z, rows, :] + part_in[place, rows, :].astype(jnp.float32)
        dw_ref[rows, :] = part_own[z, rows, :] * normalizer

    received(dx_out, o_recv)

    sent(w_all.at[pl.ds(0, (GROUP - 1) * wcols), :], w_send)
    sent(s_all.at[0, others, :], s_send)
    sent(s_all.at[0], c_send)
    sent(x_src, x_send)
    sent(x_all.at[:, others, mine], xs_send)
    sent(dx_out, o_send)
    sent(part_out.at[pl.ds(0, nz - 1)], p_send)
    for level in range(nz):
        @pl.when(z == level)
        def _():
            if level < nz - 1:
                sent(w_all.at[pl.ds(0, (level + 1) * zrows), :], g_send.at[0])
            if level > 0:
                sent(w_all.at[pl.ds(0, (nz - level) * zrows), :], g_send.at[1])


def emit(dx_ref, dw_ref, dx_out, dw_out, sems):
    for src, dst, sem in ((dx_ref, dx_out, sems.at[0]), (dw_ref, dw_out, sems.at[1])):
        rows = src.shape[0] // CHUNKS
        for i in range(CHUNKS):
            part = pl.ds(i * rows, rows)
            pltpu.make_async_copy(src.at[part, :], dst.at[part, :], sem).start()
    pltpu.make_async_copy(dx_ref, dx_out, sems.at[0]).wait()
    pltpu.make_async_copy(dw_ref, dw_out, sems.at[1]).wait()


def fused(n, inputs, value_grad, value_weight, counts, offsets):
    tok, width = inputs.shape
    half = value_grad.shape[1]
    wfeat, wcols = value_weight.shape
    nz = n // GROUP
    fq = wfeat // GROUP
    hr = width // n // 2
    bf, f32, dma = jnp.bfloat16, jnp.float32, pltpu.SemaphoreType.DMA
    normalizer = 1.0 / math.sqrt(counts.shape[1] * n)
    vmem = pl.BlockSpec(memory_space=pltpu.VMEM)
    hbm = pl.BlockSpec(memory_space=pltpu.HBM)
    held = pl.pallas_call(
        functools.partial(kernel, n, normalizer),
        out_shape=(pltpu.VMEM((tok, wfeat), bf), pltpu.VMEM((2 * hr, half), f32)),
        in_specs=[hbm] * 5,
        out_specs=(vmem, vmem),
        scratch_shapes=[
            pltpu.SMEM(counts.shape, jnp.int32),
            pltpu.SMEM(offsets.shape, jnp.int32),
            pltpu.VMEM((tok, half), bf),
            pltpu.VMEM((wcols, wfeat), bf),
            pltpu.VMEM((nz, GROUP - 1, tok, hr), bf),
            pltpu.VMEM((2, GROUP * tok, half), bf),
            pltpu.VMEM((nz, GROUP * tok, 2 * hr), bf),
            pltpu.VMEM((n * wcols, fq), bf),
            pltpu.VMEM((GROUP * tok, fq), f32),
            pltpu.VMEM((nz, 2 * hr, half), f32),
            pltpu.VMEM((nz, 2 * hr, half), bf),
            pltpu.VMEM((nz + 1, 2 * hr, half), bf),
            pltpu.VMEM((GROUP - 1, tok, fq), bf),
            dma((7,)),
            dma, dma((GROUP - 1,)),
            dma, dma((4,)),
            dma, dma,
            dma, dma((nz,)),
            dma, dma((nz,)),
            dma((2,)), dma((nz, GROUP)),
            dma, dma((nz + 1, LANES)),
            dma, dma,
            pltpu.SemaphoreType.REGULAR,
        ],
        compiler_params=pltpu.CompilerParams(
            collective_id=0, has_side_effects=True, vmem_limit_bytes=VMEM_ROOM
        ),
    )(counts, offsets, inputs, value_grad, value_weight.T)
    return pl.pallas_call(
        emit,
        out_shape=(
            jax.ShapeDtypeStruct((tok, wfeat), bf),
            jax.ShapeDtypeStruct((2 * hr, half), f32),
        ),
        in_specs=[vmem] * 2,
        out_specs=(hbm, hbm),
        scratch_shapes=[dma((2,))],
    )(*[pltpu.with_memory_space_constraint(part, pltpu.VMEM) for part in held])


def solution(mesh):
    n, tp = mesh.shape["fsdp"], mesh.shape["tp"]

    def local(inputs, value_grad, value_weight, counts, offsets):
        hr = inputs.shape[1] // n // 2
        fits = tp == 2 and n % (2 * GROUP) == 0 and n > 2 * GROUP and hr % 128 == 0
        fits = fits and value_weight.shape[1] % 16 == 0 and inputs.shape[0] % 32 == 0
        if fits:
            return fused(n, inputs, value_grad, value_weight, counts, offsets)
        return general(inputs, value_grad, value_weight, counts, offsets)

    in_specs = (P("fsdp", None), P("fsdp", "tp"), P("tp", "fsdp"), P("fsdp", None), P("fsdp", None))
    out_specs = (P("fsdp", "tp"), P("fsdp", "tp"))
    return jax.shard_map(local, mesh=mesh, in_specs=in_specs, out_specs=out_specs, check_vma=False)
```

```python
import functools
import math

import jax
import jax.numpy as jnp
from jax import lax
from jax.experimental import pallas as pl
from jax.experimental.pallas import tpu as pltpu
from jax.sharding import PartitionSpec as P

MESH = pl.DeviceIdType.MESH
GROUP = 4
LANES = 4
CHUNKS = 8
VMEM_ROOM = 54 * 2**20


def scale_rows(value_grad, counts, offsets):
    positions = jnp.arange(value_grad.shape[0], dtype=jnp.int32)[:, None]
    starts = offsets[0][None, :]
    lengths = counts[0][None, :]
    inside = (positions >= starts) & (positions < starts + lengths)
    inverse_root = lax.rsqrt(lengths.astype(jnp.float32))
    row_factor = jnp.sum(jnp.where(inside, inverse_root, jnp.zeros_like(inverse_root)), axis=1)
    return (value_grad.astype(jnp.float32) * row_factor[:, None]).astype(jnp.bfloat16)


def general(inputs, value_grad, value_weight, counts, offsets):
    tok_rows = inputs.shape[0]
    row_block = min(128, tok_rows)
    scaled = scale_rows(value_grad, counts, offsets)
    live_end = jnp.max(offsets[0] + counts[0])
    live_blocks = (live_end + row_block - 1) // row_block
    scaled_all = lax.all_gather(scaled, "tp", axis=1, tiled=True)
    empty_inputs = jnp.zeros((tok_rows, value_weight.shape[0]), jnp.float32)
    piece = lax.all_gather(value_weight, "fsdp", axis=1, tiled=True)

    def add_add_block(block_index, partial_value):
        lower = lax.dynamic_slice_in_dim(scaled_all, block_index * row_block, row_block, 0)
        before = lax.dynamic_slice_in_dim(partial_value, block_index * row_block, row_block, 0)
        product = lax.dot_general(
            lower, piece, (((1,), (1,)), ((), ())), preferred_element_type=jnp.float32
        )
        return lax.dynamic_update_slice_in_dim(
            partial_value, before + product, block_index * row_block, 0
        )

    result = lax.fori_loop(0, live_blocks, add_add_block, empty_inputs)
    input_grad = result.astype(jnp.bfloat16)
    normalizer = 1.0 / math.sqrt(counts.shape[1] * lax.axis_size("fsdp"))
    empty = jnp.zeros((inputs.shape[1], scaled.shape[1]), jnp.float32)

    def weight_add_block(block_index, partial_value):
        feature_rows = lax.dynamic_slice_in_dim(inputs, block_index * row_block, row_block, 0)
        grad_rows = lax.dynamic_slice_in_dim(scaled, block_index * row_block, row_block, 0)
        return partial_value + lax.dot_general(
            feature_rows, grad_rows, (((0,), (0,)), ((), ())), preferred_element_type=jnp.float32
        )

    result = lax.fori_loop(0, live_blocks, weight_add_block, empty)
    summed = lax.psum_scatter(result, "fsdp", scatter_dimension=0, tiled=True)
    return (input_grad, summed * normalizer)


def kernel(
    n, normalizer, counts_hbm, offsets_hbm, x_hbm, g_hbm, wt_hbm, dx_ref, dw_ref,
    counts_ref, offsets_ref, g_ref, wt_ref, x_src, s_all, x_all, w_all, acc, part_own, part_out, part_in,
    dx_out, local_sem, w_send, w_recv, s_send, s_recv, c_send, c_recv, x_send, x_recv,
    xs_send, xs_recv, g_send, g_recv, p_send, p_recv, o_send, o_recv, ready,
):
    nz = n // GROUP
    me = lax.axis_index("fsdp")
    core = lax.axis_index("tp")
    sib = 1 - core
    z = me // GROUP
    quarter = me % GROUP
    dx = 1 - 2 * (me % 2)
    dy = 2 - 4 * ((me // 2) % 2)
    steps = (0, dx, dy, dx + dy)
    tok, half = g_ref.shape
    wcols = wt_ref.shape[0]
    fq = w_all.shape[1]
    hr = x_src.shape[3]
    zrows = GROUP * wcols
    lane_rows = part_out.shape[1] // LANES
    upper = (2 * z) // nz
    order = [a + upper * (nz - 1 - 2 * a) for a in
             list(range(nz - 1, nz // 2 - 1, -1)) + list(range(nz // 2))]
    ways = ((0, 1, z < nz - 1, z > 0), (1, -1, z > 0, z < nz - 1))
    barrier = pltpu.get_barrier_semaphore()
    for j in range(1, GROUP):
        pl.semaphore_signal(barrier, inc=1, device_id=(me + steps[j], core), device_id_type=MESH)
    pl.semaphore_signal(barrier, inc=1, device_id=(me, sib), device_id_type=MESH)

    @pl.when(z < nz - 1)
    def _():
        pl.semaphore_signal(barrier, inc=1, device_id=(me + GROUP, core), device_id_type=MESH)

    def remote(src, dst, send, recv, dev):
        return pltpu.make_async_remote_copy(
            src_ref=src, dst_ref=dst, send_sem=send, recv_sem=recv,
            device_id=dev, device_id_type=MESH,
        )

    def sent(ref, sem):
        remote(ref, ref, sem, sem, (me, sib)).wait_send()

    def received(ref, sem):
        remote(ref, ref, sem, sem, (me, sib)).wait_recv()

    def w_rows(f):
        return pl.ds(pl.multiple_of(f * wcols, wcols), wcols)

    def lanes(start, size):
        return pl.ds(pl.multiple_of(start, 128), size)

    def slot(j):
        return pl.ds(j * tok, tok)

    def x_lanes(i, q, h):
        return lanes(((order[i] * GROUP + q) * 2 + h) * hr, hr)

    others = pl.ds(tok, (GROUP - 1) * tok)
    mine = lanes(core * hr, hr)

    fetch_w = pltpu.make_async_copy(wt_hbm, wt_ref, local_sem.at[0])
    fetch_own = pltpu.make_async_copy(
        wt_hbm.at[:, lanes(quarter * fq, fq)], w_all.at[w_rows(me), :], local_sem.at[1])
    fetch_g = pltpu.make_async_copy(g_hbm, g_ref, local_sem.at[2])
    fetch_counts = pltpu.make_async_copy(counts_hbm, counts_ref, local_sem.at[3])
    fetch_offsets = pltpu.make_async_copy(offsets_hbm, offsets_ref, local_sem.at[4])
    for fetch in (fetch_w, fetch_own, fetch_g, fetch_counts, fetch_offsets):
        fetch.start()
    for i in range(nz):
        for j in (3, 1, 2):
            pltpu.make_async_copy(
                x_hbm.at[:, x_lanes(i, quarter + steps[j], core)], x_src.at[i, j - 1], local_sem.at[5]).start()
    for i in range(nz):
        block_lanes = lanes((order[i] * GROUP + quarter) * 2 * hr, 2 * hr)
        pltpu.make_async_copy(x_hbm.at[:, block_lanes], x_all.at[i, slot(0), :], local_sem.at[6]).start()

    fetch_w.wait()

    @pl.when(z > 0)
    def _():
        pl.semaphore_wait(barrier, GROUP + 1)
        pl.semaphore_signal(ready, inc=1, device_id=(me - GROUP, core), device_id_type=MESH)

    @pl.when(z == 0)
    def _():
        pl.semaphore_wait(barrier, GROUP)

    for j in (3, 1, 2):
        remote(wt_ref.at[:, lanes((quarter + steps[j]) * fq, fq)], w_all.at[w_rows(me), :],
               w_send, w_recv.at[j - 1], (me + steps[j], core)).start()

    def chain(origin, way, j):
        rows = w_rows(origin * GROUP + quarter + steps[j])
        return remote(w_all.at[rows, :], w_all.at[rows, :],
                      g_send.at[(1 - way) // 2], g_recv.at[origin, j], (me + GROUP * way, core))

    def chain_pass(k, j):
        for side, way, onward, behind in ways:
            origin = z - way * k

            @pl.when((origin >= 0) & (origin < nz) & onward)
            def _():
                if k > 0:
                    chain(origin, -way, j).wait_recv()
                chain(origin, way, j).start()

    def chain_end(k):
        for side, way, onward, behind in ways:
            origin = z - way * k

            @pl.when((origin >= 0) & (origin < nz) & jnp.logical_not(onward))
            def _():
                for j in range(GROUP):
                    chain(origin, -way, j).wait_recv()

    fetch_own.wait()

    @pl.when(z > 0)
    def _():
        chain(z, -1, 0).start()

    for fetch in (fetch_g, fetch_counts, fetch_offsets):
        fetch.wait()
    positions = lax.broadcasted_iota(jnp.int32, (tok, 128), 0)
    factor = jnp.zeros((tok, 128), jnp.float32)
    for i in range(counts_ref.shape[1]):
        start = jnp.full((tok, 128), offsets_ref[0, i], jnp.int32)
        length = jnp.full((tok, 128), counts_ref[0, i], jnp.int32)
        inside = (positions >= start) & (positions < start + length)
        factor += jnp.where(inside, lax.rsqrt(length.astype(jnp.float32)), 0.0)
    for i in range(half // 128):
        cols = slice(i * 128, (i + 1) * 128)
        s_all[core, 0:tok, cols] = (g_ref[:, cols].astype(jnp.float32) * factor).astype(jnp.bfloat16)

    hop = tok // 2

    spared = hop // 4

    def s_send_rows(src_slot, dst_slot, first, count, sem, onto):
        remote(s_all.at[core, pl.ds(src_slot * tok + first, count), :],
               s_all.at[core, pl.ds(dst_slot * tok + first, count), :],
               s_send, s_recv.at[sem], (me + steps[onto], core)).start()

    for h in range(2):
        for j in (1, 2):
            s_send_rows(0, j, ((j - 1 + h) % 2) * hop, hop, 2 if h else j - 1, j)

    def to_core(first, count):
        rows = pl.ds(first * tok, count * tok)
        remote(s_all.at[core, rows, :], s_all.at[core, rows, :], c_send, c_recv, (me, sib)).start()

    to_core(0, 1)

    def x_start(i):
        for j in (3, 1, 2):
            remote(x_src.at[i, j - 1], x_all.at[i, slot(j), mine],
                   x_send, x_recv.at[i], (me + steps[j], core)).start()

    pltpu.make_async_copy(x_src, x_src, local_sem.at[5]).wait()
    x_start(0)

    @pl.when(z < nz - 1)
    def _():
        pl.semaphore_wait(ready, 1)
        chain(z, 1, 0).start()

    for j in (2, 3, 1):
        received(w_all.at[w_rows(me), :], w_recv.at[j - 1])
        chain_pass(0, j)
    received(s_all.at[core, pl.ds(0, hop), :], s_recv.at[0])
    s_send_rows(1, 3, 0, hop - spared, 3, 2)

    @pl.when(me != 2)
    def _():
        s_send_rows(1, 3, hop - spared, spared, 3, 2)

    received(s_all.at[core, pl.ds(0, hop), :], s_recv.at[1])
    s_send_rows(2, 3, hop, hop, 3, 1)
    @pl.when(me != 1)
    def _():
        for i in range(1, nz):
            x_start(i)

    for j in (0, 2, 3, 1):
        chain_pass(1, j)
    received(s_all.at[core, pl.ds(0, 2 * hop), :], s_recv.at[2])

    @pl.when(me == 1)
    def _():
        s_send_rows(2, 3, hop - spared, spared, 3, 1)
        for i in range(1, nz):
            x_start(i)

    to_core(1, 2)

    def partial_copy(t, side, lane, way, target):
        place = t if side == 0 else jnp.where(t == target, nz, t)
        rows = pl.ds(lane * lane_rows, lane_rows)
        return remote(part_out.at[t, rows, :], part_in.at[place, rows, :],
                      p_send, p_recv.at[place, lane], (me + GROUP * way, core))

    def toward(t, side):
        return t > z if side == 0 else t < z

    def x_swap(i):
        received(x_all.at[i, others, mine], x_recv.at[i])
        remote(x_all.at[i, others, mine], x_all.at[i, others, mine], xs_send, xs_recv.at[i], (me, sib)).start()

    def contract(i, rows):
        return lax.dot_general(x_all[i, rows, :], s_all[core, rows, :], (((0,), (0,)), ((), ())),
                               preferred_element_type=jnp.float32)

    def launch(i):
        t = order[i]
        for side, way, onward, behind in ways:
            @pl.when(toward(t, side) & jnp.logical_not(behind))
            def _():
                for lane in range(LANES):
                    rows = pl.ds(lane * lane_rows, lane_rows)
                    part_out[t, rows, :] = part_own[t, rows, :].astype(jnp.bfloat16)
                    partial_copy(t, side, lane, way, z + way).start()

    def block(i):
        x_swap(i)
        received(x_all.at[i, others, mine], xs_recv.at[i])
        part_own[order[i]] = contract(i, pl.ds(0, GROUP * tok))
        launch(i)

    def forward(i, lane):
        t = order[i]
        rows = pl.ds(lane * lane_rows, lane_rows)
        for side, way, onward, behind in ways:
            @pl.when(toward(t, side) & behind)
            def _():
                partial_copy(t, side, lane, -way, z).wait_recv()
                part_out[t, rows, :] = (
                    part_own[t, rows, :] + part_in[t, rows, :].astype(jnp.float32)
                ).astype(jnp.bfloat16)
                partial_copy(t, side, lane, way, z + way).start()

    pltpu.make_async_copy(x_all.at[:, slot(0), :], x_all.at[:, slot(0), :], local_sem.at[6]).wait()
    x_swap(0)
    for k in range(2, nz):
        for j in (0, 2, 3, 1):
            chain_pass(k, j)
    received(x_all.at[0, others, mine], xs_recv.at[0])
    part_own[order[0]] = contract(0, pl.ds(0, (GROUP - 1) * tok))
    received(s_all.at[core, pl.ds(0, 2 * hop), :], s_recv.at[3])
    to_core(3, 1)
    part_own[order[0]] = part_own[order[0]] + contract(0, slot(GROUP - 1))
    launch(0)

    chain_end(1)
    received(s_all.at[core], c_recv)
    near = pl.ds(pl.multiple_of(upper * half, half), half)
    far = pl.ds(pl.multiple_of((1 - upper) * half, half), half)
    for j in range(GROUP):
        acc[slot(j), :] = jnp.dot(s_all[upper, slot(j), :], w_all[near, :], preferred_element_type=jnp.float32)

    own_lanes = lanes(quarter * fq, fq)
    first = jnp.where(quarter == 1, 1, GROUP - 1)

    def give():
        for k in range(2, nz):
            chain_end(k)
        for j, step in ((first, jnp.where(quarter == 1, steps[1], steps[3])),
                        (2, steps[2]),
                        (GROUP - first, jnp.where(quarter == 1, steps[3], steps[1])), (0, None)):
            rows = pl.ds(pl.multiple_of(j * tok, tok), tok)
            product = acc[rows, :] + jnp.dot(
                s_all[1 - upper, rows, :], w_all[far, :], preferred_element_type=jnp.float32)
            if step is None:
                dx_ref[:, own_lanes] = product.astype(jnp.bfloat16)
            else:
                dx_out[j - 1] = product.astype(jnp.bfloat16)
                remote(dx_out.at[j - 1], dx_ref.at[:, own_lanes], o_send, o_recv, (me + step, core)).start()

    between = (z > 0) & (z < nz - 1)

    early = (between & (core == 0)) | ((z == 0) & (core == 1))

    @pl.when(early)
    def _():
        give()

    for lane in range(LANES):
        forward(0, lane)
    block(1)

    @pl.when(jnp.logical_not(between | early))
    def _():
        give()

    block(2)

    @pl.when(between & (core == 1))
    def _():
        give()

    for lane in range(LANES):
        forward(2, lane)
        forward(1, lane)
    for i in range(3, nz):
        block(i)
        for lane in range(LANES):
            forward(i, lane)

    for lane in range(LANES):
        rows = pl.ds(lane * lane_rows, lane_rows)
        for side, way, onward, behind in ways:
            @pl.when(behind)
            def _():
                partial_copy(z, side, lane, -way, z).wait_recv()
                place = z if side == 0 else nz
                part_own[z, rows, :] = part_own[z, rows, :] + part_in[place, rows, :].astype(jnp.float32)
        dw_ref[rows, :] = part_own[z, rows, :] * normalizer

    received(dx_out, o_recv)

    sent(w_all.at[pl.ds(0, (GROUP - 1) * wcols), :], w_send)

    @pl.when(me == 1)
    def _():
        sent(s_all.at[0, pl.ds(0, 3 * tok + spared), :], s_send)

    @pl.when(me == 2)
    def _():
        sent(s_all.at[0, pl.ds(0, 3 * tok - spared), :], s_send)

    @pl.when((me != 1) & (me != 2))
    def _():
        sent(s_all.at[0, others, :], s_send)

    sent(s_all.at[0], c_send)
    sent(x_src, x_send)
    sent(x_all.at[:, others, mine], xs_send)
    sent(dx_out, o_send)
    sent(part_out.at[pl.ds(0, nz - 1)], p_send)
    for level in range(nz):
        @pl.when(z == level)
        def _():
            if level < nz - 1:
                sent(w_all.at[pl.ds(0, (level + 1) * zrows), :], g_send.at[0])
            if level > 0:
                sent(w_all.at[pl.ds(0, (nz - level) * zrows), :], g_send.at[1])


def emit(dx_ref, dw_ref, dx_out, dw_out, sems):
    for src, dst, sem in ((dx_ref, dx_out, sems.at[0]), (dw_ref, dw_out, sems.at[1])):
        rows = src.shape[0] // CHUNKS
        for i in range(CHUNKS):
            part = pl.ds(i * rows, rows)
            pltpu.make_async_copy(src.at[part, :], dst.at[part, :], sem).start()
    pltpu.make_async_copy(dx_ref, dx_out, sems.at[0]).wait()
    pltpu.make_async_copy(dw_ref, dw_out, sems.at[1]).wait()


def fused(n, inputs, value_grad, value_weight, counts, offsets):
    tok, width = inputs.shape
    half = value_grad.shape[1]
    wfeat, wcols = value_weight.shape
    nz = n // GROUP
    fq = wfeat // GROUP
    hr = width // n // 2
    bf, f32, dma = jnp.bfloat16, jnp.float32, pltpu.SemaphoreType.DMA
    normalizer = 1.0 / math.sqrt(counts.shape[1] * n)
    vmem = pl.BlockSpec(memory_space=pltpu.VMEM)
    hbm = pl.BlockSpec(memory_space=pltpu.HBM)
    held = pl.pallas_call(
        functools.partial(kernel, n, normalizer),
        out_shape=(pltpu.VMEM((tok, wfeat), bf), pltpu.VMEM((2 * hr, half), f32)),
        in_specs=[hbm] * 5,
        out_specs=(vmem, vmem),
        scratch_shapes=[
            pltpu.SMEM(counts.shape, jnp.int32),
            pltpu.SMEM(offsets.shape, jnp.int32),
            pltpu.VMEM((tok, half), bf),
            pltpu.VMEM((wcols, wfeat), bf),
            pltpu.VMEM((nz, GROUP - 1, tok, hr), bf),
            pltpu.VMEM((2, GROUP * tok, half), bf),
            pltpu.VMEM((nz, GROUP * tok, 2 * hr), bf),
            pltpu.VMEM((n * wcols, fq), bf),
            pltpu.VMEM((GROUP * tok, fq), f32),
            pltpu.VMEM((nz, 2 * hr, half), f32),
            pltpu.VMEM((nz, 2 * hr, half), bf),
            pltpu.VMEM((nz + 1, 2 * hr, half), bf),
            pltpu.VMEM((GROUP - 1, tok, fq), bf),
            dma((7,)),
            dma, dma((GROUP - 1,)),
            dma, dma((4,)),
            dma, dma,
            dma, dma((nz,)),
            dma, dma((nz,)),
            dma((2,)), dma((nz, GROUP)),
            dma, dma((nz + 1, LANES)),
            dma, dma,
            pltpu.SemaphoreType.REGULAR,
        ],
        compiler_params=pltpu.CompilerParams(
            collective_id=0, has_side_effects=True, vmem_limit_bytes=VMEM_ROOM
        ),
    )(counts, offsets, inputs, value_grad, value_weight.T)
    return pl.pallas_call(
        emit,
        out_shape=(
            jax.ShapeDtypeStruct((tok, wfeat), bf),
            jax.ShapeDtypeStruct((2 * hr, half), f32),
        ),
        in_specs=[vmem] * 2,
        out_specs=(hbm, hbm),
        scratch_shapes=[dma((2,))],
    )(*[pltpu.with_memory_space_constraint(part, pltpu.VMEM) for part in held])


def solution(mesh):
    n, tp = mesh.shape["fsdp"], mesh.shape["tp"]

    def local(inputs, value_grad, value_weight, counts, offsets):
        hr = inputs.shape[1] // n // 2
        fits = tp == 2 and n % (2 * GROUP) == 0 and n > 2 * GROUP and hr % 128 == 0
        fits = fits and value_weight.shape[1] % 16 == 0 and inputs.shape[0] % 32 == 0
        if fits:
            return fused(n, inputs, value_grad, value_weight, counts, offsets)
        return general(inputs, value_grad, value_weight, counts, offsets)

    in_specs = (P("fsdp", None), P("fsdp", "tp"), P("tp", "fsdp"), P("fsdp", None), P("fsdp", None))
    out_specs = (P("fsdp", "tp"), P("fsdp", "tp"))
    return jax.shard_map(local, mesh=mesh, in_specs=in_specs, out_specs=out_specs, check_vma=False)
```

```python
import functools
import math

import jax
import jax.numpy as jnp
from jax import lax
from jax.experimental import pallas as pl
from jax.experimental.pallas import tpu as pltpu
from jax.sharding import PartitionSpec as P

MESH = pl.DeviceIdType.MESH
GROUP = 4
LANES = 4
CHUNKS = 8
VMEM_ROOM = 54 * 2**20


def scale_rows(value_grad, counts, offsets):
    positions = jnp.arange(value_grad.shape[0], dtype=jnp.int32)[:, None]
    starts = offsets[0][None, :]
    lengths = counts[0][None, :]
    inside = (positions >= starts) & (positions < starts + lengths)
    inverse_root = lax.rsqrt(lengths.astype(jnp.float32))
    row_factor = jnp.sum(jnp.where(inside, inverse_root, jnp.zeros_like(inverse_root)), axis=1)
    return (value_grad.astype(jnp.float32) * row_factor[:, None]).astype(jnp.bfloat16)


def general(inputs, value_grad, value_weight, counts, offsets):
    tok_rows = inputs.shape[0]
    row_block = min(128, tok_rows)
    scaled = scale_rows(value_grad, counts, offsets)
    live_end = jnp.max(offsets[0] + counts[0])
    live_blocks = (live_end + row_block - 1) // row_block
    scaled_all = lax.all_gather(scaled, "tp", axis=1, tiled=True)
    empty_inputs = jnp.zeros((tok_rows, value_weight.shape[0]), jnp.float32)
    piece = lax.all_gather(value_weight, "fsdp", axis=1, tiled=True)

    def add_add_block(block_index, partial_value):
        lower = lax.dynamic_slice_in_dim(scaled_all, block_index * row_block, row_block, 0)
        before = lax.dynamic_slice_in_dim(partial_value, block_index * row_block, row_block, 0)
        product = lax.dot_general(
            lower, piece, (((1,), (1,)), ((), ())), preferred_element_type=jnp.float32
        )
        return lax.dynamic_update_slice_in_dim(
            partial_value, before + product, block_index * row_block, 0
        )

    result = lax.fori_loop(0, live_blocks, add_add_block, empty_inputs)
    input_grad = result.astype(jnp.bfloat16)
    normalizer = 1.0 / math.sqrt(counts.shape[1] * lax.axis_size("fsdp"))
    empty = jnp.zeros((inputs.shape[1], scaled.shape[1]), jnp.float32)

    def weight_add_block(block_index, partial_value):
        feature_rows = lax.dynamic_slice_in_dim(inputs, block_index * row_block, row_block, 0)
        grad_rows = lax.dynamic_slice_in_dim(scaled, block_index * row_block, row_block, 0)
        return partial_value + lax.dot_general(
            feature_rows, grad_rows, (((0,), (0,)), ((), ())), preferred_element_type=jnp.float32
        )

    result = lax.fori_loop(0, live_blocks, weight_add_block, empty)
    summed = lax.psum_scatter(result, "fsdp", scatter_dimension=0, tiled=True)
    return (input_grad, summed * normalizer)


def kernel(
    n, normalizer, counts_hbm, offsets_hbm, x_hbm, g_hbm, wt_hbm, dx_ref, dw_ref,
    counts_ref, offsets_ref, g_ref, wt_ref, x_src, s_all, x_all, w_all, acc, part_own, part_out, part_in,
    dx_out, local_sem, w_send, w_recv, s_send, s_recv, c_send, c_recv, x_send, x_recv,
    xs_send, xs_recv, g_send, g_recv, p_send, p_recv, o_send, o_recv, ready,
):
    nz = n // GROUP
    me = lax.axis_index("fsdp")
    core = lax.axis_index("tp")
    sib = 1 - core
    z = me // GROUP
    quarter = me % GROUP
    dx = 1 - 2 * (me % 2)
    dy = 2 - 4 * ((me // 2) % 2)
    steps = (0, dx, dy, dx + dy)
    tok, half = g_ref.shape
    wcols = wt_ref.shape[0]
    fq = w_all.shape[1]
    hr = x_src.shape[3]
    zrows = GROUP * wcols
    lane_rows = part_out.shape[1] // LANES
    upper = (2 * z) // nz
    order = [a + upper * (nz - 1 - 2 * a) for a in
             list(range(nz - 1, nz // 2 - 1, -1)) + list(range(nz // 2))]
    ways = ((0, 1, z < nz - 1, z > 0), (1, -1, z > 0, z < nz - 1))
    barrier = pltpu.get_barrier_semaphore()
    for j in range(1, GROUP):
        pl.semaphore_signal(barrier, inc=1, device_id=(me + steps[j], core), device_id_type=MESH)
    pl.semaphore_signal(barrier, inc=1, device_id=(me, sib), device_id_type=MESH)

    @pl.when(z < nz - 1)
    def _():
        pl.semaphore_signal(barrier, inc=1, device_id=(me + GROUP, core), device_id_type=MESH)

    def remote(src, dst, send, recv, dev):
        return pltpu.make_async_remote_copy(
            src_ref=src, dst_ref=dst, send_sem=send, recv_sem=recv,
            device_id=dev, device_id_type=MESH,
        )

    def sent(ref, sem):
        remote(ref, ref, sem, sem, (me, sib)).wait_send()

    def received(ref, sem):
        remote(ref, ref, sem, sem, (me, sib)).wait_recv()

    def w_rows(f):
        return pl.ds(pl.multiple_of(f * wcols, wcols), wcols)

    def lanes(start, size):
        return pl.ds(pl.multiple_of(start, 128), size)

    def slot(j):
        return pl.ds(j * tok, tok)

    def x_lanes(i, q, h):
        return lanes(((order[i] * GROUP + q) * 2 + h) * hr, hr)

    others = pl.ds(tok, (GROUP - 1) * tok)
    mine = lanes(core * hr, hr)

    fetch_w = pltpu.make_async_copy(wt_hbm, wt_ref, local_sem.at[0])
    fetch_own = pltpu.make_async_copy(
        wt_hbm.at[:, lanes(quarter * fq, fq)], w_all.at[w_rows(me), :], local_sem.at[1])
    fetch_g = pltpu.make_async_copy(g_hbm, g_ref, local_sem.at[2])
    fetch_counts = pltpu.make_async_copy(counts_hbm, counts_ref, local_sem.at[3])
    fetch_offsets = pltpu.make_async_copy(offsets_hbm, offsets_ref, local_sem.at[4])
    for fetch in (fetch_w, fetch_own, fetch_g, fetch_counts, fetch_offsets):
        fetch.start()
    for i in range(nz):
        for j in (3, 1, 2):
            pltpu.make_async_copy(
                x_hbm.at[:, x_lanes(i, quarter + steps[j], core)], x_src.at[i, j - 1], local_sem.at[5]).start()
    for i in range(nz):
        block_lanes = lanes((order[i] * GROUP + quarter) * 2 * hr, 2 * hr)
        pltpu.make_async_copy(x_hbm.at[:, block_lanes], x_all.at[i, slot(0), :], local_sem.at[6]).start()

    fetch_w.wait()

    @pl.when(z > 0)
    def _():
        pl.semaphore_wait(barrier, GROUP + 1)
        pl.semaphore_signal(ready, inc=1, device_id=(me - GROUP, core), device_id_type=MESH)

    @pl.when(z == 0)
    def _():
        pl.semaphore_wait(barrier, GROUP)

    for j in (3, 1, 2):
        remote(wt_ref.at[:, lanes((quarter + steps[j]) * fq, fq)], w_all.at[w_rows(me), :],
               w_send, w_recv.at[j - 1], (me + steps[j], core)).start()

    def chain(origin, way, j):
        rows = w_rows(origin * GROUP + quarter + steps[j])
        return remote(w_all.at[rows, :], w_all.at[rows, :],
                      g_send.at[(1 - way) // 2], g_recv.at[origin, j], (me + GROUP * way, core))

    def chain_pass(k, j):
        for side, way, onward, behind in ways:
            origin = z - way * k

            @pl.when((origin >= 0) & (origin < nz) & onward)
            def _():
                if k > 0:
                    chain(origin, -way, j).wait_recv()
                chain(origin, way, j).start()

    def chain_end(k):
        for side, way, onward, behind in ways:
            origin = z - way * k

            @pl.when((origin >= 0) & (origin < nz) & jnp.logical_not(onward))
            def _():
                for j in range(GROUP):
                    chain(origin, -way, j).wait_recv()

    fetch_own.wait()

    @pl.when(z > 0)
    def _():
        chain(z, -1, 0).start()

    for fetch in (fetch_g, fetch_counts, fetch_offsets):
        fetch.wait()
    positions = lax.broadcasted_iota(jnp.int32, (tok, 128), 0)
    factor = jnp.zeros((tok, 128), jnp.float32)
    for i in range(counts_ref.shape[1]):
        start = jnp.full((tok, 128), offsets_ref[0, i], jnp.int32)
        length = jnp.full((tok, 128), counts_ref[0, i], jnp.int32)
        inside = (positions >= start) & (positions < start + length)
        factor += jnp.where(inside, lax.rsqrt(length.astype(jnp.float32)), 0.0)
    for i in range(half // 128):
        cols = slice(i * 128, (i + 1) * 128)
        s_all[core, 0:tok, cols] = (g_ref[:, cols].astype(jnp.float32) * factor).astype(jnp.bfloat16)

    hop = tok // 2

    spared = hop // 4

    def s_send_rows(src_slot, dst_slot, first, count, sem, onto):
        remote(s_all.at[core, pl.ds(src_slot * tok + first, count), :],
               s_all.at[core, pl.ds(dst_slot * tok + first, count), :],
               s_send, s_recv.at[sem], (me + steps[onto], core)).start()

    for h in range(2):
        for j in (1, 2):
            s_send_rows(0, j, ((j - 1 + h) % 2) * hop, hop, 2 if h else j - 1, j)

    def to_core(first, count):
        rows = pl.ds(first * tok, count * tok)
        remote(s_all.at[core, rows, :], s_all.at[core, rows, :], c_send, c_recv, (me, sib)).start()

    to_core(0, 1)

    def x_start(i):
        for j in (3, 1, 2):
            remote(x_src.at[i, j - 1], x_all.at[i, slot(j), mine],
                   x_send, x_recv.at[i], (me + steps[j], core)).start()

    pltpu.make_async_copy(x_src, x_src, local_sem.at[5]).wait()
    x_start(0)

    @pl.when(z < nz - 1)
    def _():
        pl.semaphore_wait(ready, 1)
        chain(z, 1, 0).start()

    for j in (2, 3, 1):
        received(w_all.at[w_rows(me), :], w_recv.at[j - 1])
        chain_pass(0, j)
    received(s_all.at[core, pl.ds(0, hop), :], s_recv.at[0])
    s_send_rows(1, 3, 0, hop - spared, 3, 2)

    @pl.when(me != 2)
    def _():
        s_send_rows(1, 3, hop - spared, spared, 3, 2)

    received(s_all.at[core, pl.ds(0, hop), :], s_recv.at[1])
    s_send_rows(2, 3, hop, hop, 3, 1)
    @pl.when(me != 1)
    def _():
        for i in range(1, nz):
            x_start(i)

    for j in (0, 2, 3, 1):
        chain_pass(1, j)
    received(s_all.at[core, pl.ds(0, 2 * hop), :], s_recv.at[2])

    @pl.when(me == 1)
    def _():
        s_send_rows(2, 3, hop - spared, spared, 3, 1)
        for i in range(1, nz):
            x_start(i)

    to_core(1, 2)

    def partial_copy(t, side, lane, way, target):
        place = t if side == 0 else jnp.where(t == target, nz, t)
        rows = pl.ds(lane * lane_rows, lane_rows)
        return remote(part_out.at[t, rows, :], part_in.at[place, rows, :],
                      p_send, p_recv.at[place, lane], (me + GROUP * way, core))

    def toward(t, side):
        return t > z if side == 0 else t < z

    def x_swap(i):
        received(x_all.at[i, others, mine], x_recv.at[i])
        remote(x_all.at[i, others, mine], x_all.at[i, others, mine], xs_send, xs_recv.at[i], (me, sib)).start()

    def contract(i, rows):
        return lax.dot_general(x_all[i, rows, :], s_all[core, rows, :], (((0,), (0,)), ((), ())),
                               preferred_element_type=jnp.float32)

    def launch(i):
        t = order[i]
        for side, way, onward, behind in ways:
            @pl.when(toward(t, side) & jnp.logical_not(behind))
            def _():
                for lane in range(LANES):
                    rows = pl.ds(lane * lane_rows, lane_rows)
                    part_out[t, rows, :] = part_own[t, rows, :].astype(jnp.bfloat16)
                    partial_copy(t, side, lane, way, z + way).start()

    def block(i):
        x_swap(i)
        received(x_all.at[i, others, mine], xs_recv.at[i])
        part_own[order[i]] = contract(i, pl.ds(0, GROUP * tok))
        launch(i)

    def forward(i, lane):
        t = order[i]
        rows = pl.ds(lane * lane_rows, lane_rows)
        for side, way, onward, behind in ways:
            @pl.when(toward(t, side) & behind)
            def _():
                partial_copy(t, side, lane, -way, z).wait_recv()
                part_out[t, rows, :] = (
                    part_own[t, rows, :] + part_in[t, rows, :].astype(jnp.float32)
                ).astype(jnp.bfloat16)
                partial_copy(t, side, lane, way, z + way).start()

    pltpu.make_async_copy(x_all.at[:, slot(0), :], x_all.at[:, slot(0), :], local_sem.at[6]).wait()
    x_swap(0)
    for k in range(2, nz):
        for j in (0, 2, 3, 1):
            chain_pass(k, j)
    received(x_all.at[0, others, mine], xs_recv.at[0])
    part_own[order[0]] = contract(0, pl.ds(0, (GROUP - 1) * tok))
    received(s_all.at[core, pl.ds(0, 2 * hop), :], s_recv.at[3])
    to_core(3, 1)
    part_own[order[0]] = part_own[order[0]] + contract(0, slot(GROUP - 1))
    launch(0)

    chain_end(1)
    received(s_all.at[core], c_recv)
    near = pl.ds(pl.multiple_of(upper * half, half), half)
    far = pl.ds(pl.multiple_of((1 - upper) * half, half), half)
    for j in range(GROUP):
        acc[slot(j), :] = jnp.dot(s_all[upper, slot(j), :], w_all[near, :], preferred_element_type=jnp.float32)

    own_lanes = lanes(quarter * fq, fq)
    first = jnp.where(quarter == 1, 1, GROUP - 1)

    def give():
        for k in range(2, nz):
            chain_end(k)
        for j, step in ((first, jnp.where(quarter == 1, steps[1], steps[3])),
                        (2, steps[2]),
                        (GROUP - first, jnp.where(quarter == 1, steps[3], steps[1])), (0, None)):
            rows = pl.ds(pl.multiple_of(j * tok, tok), tok)
            product = acc[rows, :] + jnp.dot(
                s_all[1 - upper, rows, :], w_all[far, :], preferred_element_type=jnp.float32)
            if step is None:
                dx_ref[:, own_lanes] = product.astype(jnp.bfloat16)
            else:
                dx_out[j - 1] = product.astype(jnp.bfloat16)
                remote(dx_out.at[j - 1], dx_ref.at[:, own_lanes], o_send, o_recv, (me + step, core)).start()

    between = (z > 0) & (z < nz - 1)

    early = (between & (core == 0)) | ((z == 0) & (core == 1))

    @pl.when(early)
    def _():
        give()

    for lane in range(LANES):
        forward(0, lane)
    block(1)

    @pl.when(jnp.logical_not(between | early))
    def _():
        give()

    block(2)

    @pl.when(between & (core == 1))
    def _():
        give()

    for lane in range(LANES):
        forward(2, lane)
        forward(1, lane)
    for i in range(3, nz):
        block(i)
        for lane in range(LANES):
            forward(i, lane)

    sent(w_all.at[pl.ds(0, (GROUP - 1) * wcols), :], w_send)

    @pl.when(me == 1)
    def _():
        sent(s_all.at[0, pl.ds(0, 3 * tok + spared), :], s_send)

    @pl.when(me == 2)
    def _():
        sent(s_all.at[0, pl.ds(0, 3 * tok - spared), :], s_send)

    @pl.when((me != 1) & (me != 2))
    def _():
        sent(s_all.at[0, others, :], s_send)

    sent(s_all.at[0], c_send)
    sent(x_src, x_send)
    sent(x_all.at[:, others, mine], xs_send)
    for level in range(nz):
        @pl.when(z == level)
        def _():
            if level < nz - 1:
                sent(w_all.at[pl.ds(0, (level + 1) * zrows), :], g_send.at[0])
            if level > 0:
                sent(w_all.at[pl.ds(0, (nz - level) * zrows), :], g_send.at[1])

    for lane in range(LANES):
        rows = pl.ds(lane * lane_rows, lane_rows)
        for side, way, onward, behind in ways:
            @pl.when(behind)
            def _():
                partial_copy(z, side, lane, -way, z).wait_recv()
                place = z if side == 0 else nz
                part_own[z, rows, :] = part_own[z, rows, :] + part_in[place, rows, :].astype(jnp.float32)
        dw_ref[rows, :] = part_own[z, rows, :] * normalizer

    sent(part_out.at[pl.ds(0, nz - 1)], p_send)
    received(dx_out, o_recv)

    sent(dx_out, o_send)


def emit(dx_ref, dw_ref, dx_out, dw_out, sems):
    for src, dst, sem in ((dx_ref, dx_out, sems.at[0]), (dw_ref, dw_out, sems.at[1])):
        rows = src.shape[0] // CHUNKS
        for i in range(CHUNKS):
            part = pl.ds(i * rows, rows)
            pltpu.make_async_copy(src.at[part, :], dst.at[part, :], sem).start()
    pltpu.make_async_copy(dx_ref, dx_out, sems.at[0]).wait()
    pltpu.make_async_copy(dw_ref, dw_out, sems.at[1]).wait()


def fused(n, inputs, value_grad, value_weight, counts, offsets):
    tok, width = inputs.shape
    half = value_grad.shape[1]
    wfeat, wcols = value_weight.shape
    nz = n // GROUP
    fq = wfeat // GROUP
    hr = width // n // 2
    bf, f32, dma = jnp.bfloat16, jnp.float32, pltpu.SemaphoreType.DMA
    normalizer = 1.0 / math.sqrt(counts.shape[1] * n)
    vmem = pl.BlockSpec(memory_space=pltpu.VMEM)
    hbm = pl.BlockSpec(memory_space=pltpu.HBM)
    held = pl.pallas_call(
        functools.partial(kernel, n, normalizer),
        out_shape=(pltpu.VMEM((tok, wfeat), bf), pltpu.VMEM((2 * hr, half), f32)),
        in_specs=[hbm] * 5,
        out_specs=(vmem, vmem),
        scratch_shapes=[
            pltpu.SMEM(counts.shape, jnp.int32),
            pltpu.SMEM(offsets.shape, jnp.int32),
            pltpu.VMEM((tok, half), bf),
            pltpu.VMEM((wcols, wfeat), bf),
            pltpu.VMEM((nz, GROUP - 1, tok, hr), bf),
            pltpu.VMEM((2, GROUP * tok, half), bf),
            pltpu.VMEM((nz, GROUP * tok, 2 * hr), bf),
            pltpu.VMEM((n * wcols, fq), bf),
            pltpu.VMEM((GROUP * tok, fq), f32),
            pltpu.VMEM((nz, 2 * hr, half), f32),
            pltpu.VMEM((nz, 2 * hr, half), bf),
            pltpu.VMEM((nz + 1, 2 * hr, half), bf),
            pltpu.VMEM((GROUP - 1, tok, fq), bf),
            dma((7,)),
            dma, dma((GROUP - 1,)),
            dma, dma((4,)),
            dma, dma,
            dma, dma((nz,)),
            dma, dma((nz,)),
            dma((2,)), dma((nz, GROUP)),
            dma, dma((nz + 1, LANES)),
            dma, dma,
            pltpu.SemaphoreType.REGULAR,
        ],
        compiler_params=pltpu.CompilerParams(
            collective_id=0, has_side_effects=True, vmem_limit_bytes=VMEM_ROOM
        ),
    )(counts, offsets, inputs, value_grad, value_weight.T)
    return pl.pallas_call(
        emit,
        out_shape=(
            jax.ShapeDtypeStruct((tok, wfeat), bf),
            jax.ShapeDtypeStruct((2 * hr, half), f32),
        ),
        in_specs=[vmem] * 2,
        out_specs=(hbm, hbm),
        scratch_shapes=[dma((2,))],
    )(*[pltpu.with_memory_space_constraint(part, pltpu.VMEM) for part in held])


def solution(mesh):
    n, tp = mesh.shape["fsdp"], mesh.shape["tp"]

    def local(inputs, value_grad, value_weight, counts, offsets):
        hr = inputs.shape[1] // n // 2
        fits = tp == 2 and n % (2 * GROUP) == 0 and n > 2 * GROUP and hr % 128 == 0
        fits = fits and value_weight.shape[1] % 16 == 0 and inputs.shape[0] % 32 == 0
        if fits:
            return fused(n, inputs, value_grad, value_weight, counts, offsets)
        return general(inputs, value_grad, value_weight, counts, offsets)

    in_specs = (P("fsdp", None), P("fsdp", "tp"), P("tp", "fsdp"), P("fsdp", None), P("fsdp", None))
    out_specs = (P("fsdp", "tp"), P("fsdp", "tp"))
    return jax.shard_map(local, mesh=mesh, in_specs=in_specs, out_specs=out_specs, check_vma=False)
```
